256 devices in a mesh: block: 8 (over z_lo, x_lo, core), span: 4 (over z_hi), model: 8 (over y, x_hi).
Axes of the slice: x: 4 (x_hi: 2, x_lo: 2; x = x_hi * 2 + x_lo), y: 4, z: 8 (z_hi: 4, z_lo: 2; z = z_hi * 2 + z_lo), core: 2. Of those that a mesh axis runs over, the one named last changes fastest.
Arguments:
- fresh_keys: bfloat16 [32, 16384, 8, 128], P(None, ('block', 'span'), 'model'), may hold values from -6 to 6
- fresh_values: bfloat16 [32, 16384, 8, 128], P(None, ('block', 'span'), 'model'), may hold values from -6 to 6
- turn_angle: float32 [16384, 64], replicated, may hold values from -3.140625 to 3.140625
Outputs:
- decode_keys: bfloat16 [32, 8, 128, 16384], P(('block', 'span'), 'model')
- decode_values: bfloat16 [32, 16384, 8, 128], P(('block', 'span'), None, 'model')
- page_high: bfloat16 [32, 256, 8, 128], P(('block', 'span'), None, 'model')
- page_low: bfloat16 [32, 256, 8, 128], P(('block', 'span'), None, 'model')
The draws below stay inside these ranges and needn't reach their ends.
All inputs are finite; a program needn't handle non-finite values.
Results may differ from the reference program's by a relative error of at most 0.001.
Values may be sent and summed in bfloat16 or wider, within the bound.
A program may use at most 128 MiB of HBM per device.

```python
import jax
import jax.numpy as jnp

BATCH = 32
LENGTH = 16384
KV_HEADS = 8
HEAD_SIZE = 128
HALF_HEAD = 64
PAGE = 64


def level_of(own_key, dims, split, smallest, high):
    def one(axis_at, blocks):
        draws = jax.random.uniform(jax.random.fold_in(jax.random.fold_in(own_key, 6), axis_at), (blocks,), jnp.float32, smallest / len(split), high / len(split))
        return jnp.repeat(jnp.exp(draws), dims[axis_at] // blocks).reshape((-1,) + (1,) * (len(dims) - axis_at - 1))

    gain = one(*split[0])
    for cut in split[1:]:
        gain = gain * one(*cut)
    return gain


def noise(stream_key, shape, deviation, most, split=(), held_as=jnp.bfloat16):
    result = deviation * jax.random.normal(stream_key, shape, jnp.float32)
    if split:
        result = result * level_of(stream_key, shape, split, -0.22, 0.18)
    return jnp.clip(result, -most, most).astype(held_as)


def setup_inputs(seed: int = 0) -> dict:
    seeds = jax.random.split(jax.random.key(seed), 4)
    return {
        "fresh_keys": noise(seeds[0], (BATCH, LENGTH, KV_HEADS, HEAD_SIZE), 1.0, 6.0, ((1, 32), (2, 8))),
        "fresh_values": noise(seeds[1], (BATCH, LENGTH, KV_HEADS, HEAD_SIZE), 1.0, 6.0, ((1, 32), (2, 8))),
        "turn_angle": jnp.clip(jax.random.uniform(seeds[2], (LENGTH, HALF_HEAD), jnp.float32, -3.140625, 3.140625), -3.140625, 3.140625),
    }


def apply_rotary(vectors, angle):
    half = vectors.shape[-1] // 2
    cosine, sine = jnp.cos(angle)[None, :, None, :], jnp.sin(angle)[None, :, None, :]
    first, second = vectors[..., :half], vectors[..., half:]
    return jnp.concatenate([first * cosine - second * sine, second * cosine + first * sine], axis=-1)


def ready_to_store(plain_keys, angle):
    wide_keys = plain_keys.astype(jnp.float32)
    return apply_rotary(wide_keys, angle)


def reference(fresh_keys, fresh_values, turn_angle):
    turned_keys = ready_to_store(fresh_keys, turn_angle)
    narrow_keys = turned_keys.astype(jnp.bfloat16)
    page_view = narrow_keys.reshape(BATCH, LENGTH // PAGE, PAGE, KV_HEADS, HEAD_SIZE)
    page_high = jnp.max(page_view, axis=2)
    page_low = jnp.min(page_view, axis=2)
    decode_keys = jnp.transpose(narrow_keys, (0, 2, 3, 1))
    decode_values = fresh_values
    return decode_keys, decode_values, page_high, page_low
```

```python
import functools

import jax
import jax.numpy as jnp
from jax import lax
from jax.experimental import pallas as pl
from jax.experimental.pallas import tpu as pltpu
from jax.sharding import PartitionSpec as P

PAGE = 64
MESH = pl.DeviceIdType.MESH
RING = 8
STEPS = (1, 7, 2, 6, 3, 5, 4)
ALONG = tuple((dz, dc) for dz in STEPS for dc in range(2))


def place(core, x, z, model):
    return ((z % 2) * 4 + x * 2 + core, z // 2, model)


def rank(core, x, z):
    return ((z % 2) * 4 + x * 2 + core) * 4 + z // 2


def exchange(
    keys, values, angle, out_keys, out_values, out_high, out_low,
    plain, turned, landed, relay, angles, cosine, sine, high, low,
    load_sem, send_sem, recv_sem, pass_send_sem, pass_recv_sem,
):
    block, span, model = (lax.axis_index(a) for a in ("block", "span", "model"))
    core, x, z = block % 2, (block // 2) % 2, span * 2 + block // 4
    me = rank(core, x, z)
    count, rows, size = plain.shape
    pages = rows // PAGE
    half = size // 2

    def remote(src, dst, ssem, rsem, to):
        return pltpu.make_async_remote_copy(
            src, dst, ssem, rsem, device_id=place(*to, model), device_id_type=MESH
        )

    def rows_of(r):
        return pl.ds(pl.multiple_of(r * rows, rows), rows)

    barrier = pltpu.get_barrier_semaphore()
    peers = [((core + dc) % 2, x, (z + dz) % RING) for dz, dc in ALONG]
    mate = (1 - core, x, z)
    across = [(c, 1 - x, z) for c in (core, 1 - core)]
    for to in peers + [mate] + across:
        pl.semaphore_signal(barrier, inc=1, device_id=place(*to, model), device_id_type=MESH)

    get_angle = pltpu.make_async_copy(angle.at[:, rows_of(me)], angles, load_sem.at[0])
    get_angle.start()
    get_keys = pltpu.make_async_copy(keys, plain, load_sem.at[1])
    get_keys.start()
    put_own = pltpu.make_async_copy(values.at[me], out_values.at[rows_of(me)], load_sem.at[2])
    put_own.start()

    n = len(ALONG)
    def along(kind, i):
        to = peers[i]
        c2, _, z2 = to
        final = rank(c2, 1 - x if kind < 2 else x, z2)
        src = (values if kind in (0, 3) else turned).at[final]
        if kind < 2:
            dst = relay.at[kind, i]
        elif kind == 2:
            dst = landed.at[me]
        else:
            dst = out_values.at[rows_of(me)]
        return remote(src, dst, send_sem.at[kind * n + i], recv_sem.at[kind * n + i], to)

    def beside(i, what):
        to = ([mate] + across)[i]
        at = 4 * n + what * 3 + i
        src = (values if what == 0 else turned).at[rank(*to)]
        dst = out_values.at[rows_of(me)] if what == 0 else landed.at[me]
        return remote(src, dst, send_sem.at[at], recv_sem.at[at], to)

    def passed(kind, i):
        dz, dc = ALONG[i]
        origin = rank((core - dc) % 2, x, (z - dz) % RING)
        dst = out_values.at[rows_of(origin)] if kind == 0 else landed.at[origin]
        return remote(
            relay.at[kind, i], dst, pass_send_sem.at[kind * n + i], pass_recv_sem.at[kind * n + i],
            across[0],
        )

    get_angle.wait()
    a = angles[...]
    ca, sa = jnp.cos(a), jnp.sin(a)
    cosine[...] = jnp.concatenate([ca, ca], axis=0).T
    sine[...] = jnp.concatenate([-sa, sa], axis=0).T

    pl.semaphore_wait(barrier, n + 3)
    for i in range(n):
        along(0, i).start()
    for i in range(3):
        beside(i, 0).start()

    get_keys.wait()
    part = 128

    def turn(j, _):
        s = j // (rows // part)
        r = pl.ds(pl.multiple_of((j % (rows // part)) * part, part), part)
        v = plain[s, r, :].astype(jnp.float32)
        w = v * cosine[r, :] + pltpu.roll(v, half, 1) * sine[r, :]
        turned[s, r, :] = w.astype(jnp.bfloat16)
        return 0

    lax.fori_loop(0, count * (rows // part), turn, 0)

    def finish(ref, s, origin):
        v = ref[s]
        out_keys[:, rows_of(origin)] = v.T
        g = v.astype(jnp.float32).reshape(pages, PAGE, size)
        at = pl.ds(pl.multiple_of(origin * pages, pages), pages)
        high[at, :] = jnp.max(g, axis=1)
        low[at, :] = jnp.min(g, axis=1)

    finish(turned, me, me)
    for kind in (1, 2):
        for i in range(n):
            along(kind, i).start()
    for i in range(3):
        beside(i, 1).start()
    for i in range(n):
        along(3, i).start()

    for kind in (0, 1):
        for i in range(n):
            along(kind, i).wait_recv()
            passed(kind, i).start()

    def arrive(i, _):
        pass

    def origin_of(i, col):
        dz, dc = ALONG[i]
        return rank((core - dc) % 2, col, (z - dz) % RING)

    for i in range(3):
        beside(i, 1).wait_recv()
        finish(landed, rank(*([mate] + across)[i]), rank(*([mate] + across)[i]))
    for i in range(n):
        along(2, i).wait_recv()
        o = origin_of(i, x)
        finish(landed, o, o)
    for i in range(n):
        passed(1, i).wait_recv()
        o = origin_of(i, 1 - x)
        finish(landed, o, o)
    out_high[...] = high[...].astype(jnp.bfloat16)
    out_low[...] = low[...].astype(jnp.bfloat16)

    put_own.wait()
    for i in range(3):
        beside(i, 0).wait_recv()
    for i in range(n):
        passed(0, i).wait_recv()
    for i in range(n):
        along(3, i).wait_recv()
    for kind in range(4):
        for i in range(n):
            along(kind, i).wait_send()
    for what in range(2):
        for i in range(3):
            beside(i, what).wait_send()
    for kind in range(2):
        for i in range(n):
            passed(kind, i).wait_send()


def body(fresh_keys, fresh_values, turn_angle):
    count, rows, _, size = fresh_keys.shape
    length = count * rows
    n = len(ALONG)
    plain = (count, rows, size)
    vmem = pl.BlockSpec(memory_space=pltpu.VMEM)
    hbm = pl.BlockSpec(memory_space=pltpu.HBM)
    out = pl.pallas_call(
        exchange,
        out_shape=[
            jax.ShapeDtypeStruct((size, length), jnp.bfloat16),
            jax.ShapeDtypeStruct((length, size), jnp.bfloat16),
            jax.ShapeDtypeStruct((length // PAGE, size), jnp.bfloat16),
            jax.ShapeDtypeStruct((length // PAGE, size), jnp.bfloat16),
        ],
        in_specs=[hbm] * 3,
        out_specs=[vmem] * 4,
        scratch_shapes=[
            pltpu.VMEM(plain, jnp.bfloat16),
            pltpu.VMEM(plain, jnp.bfloat16),
            pltpu.VMEM(plain, jnp.bfloat16),
            pltpu.VMEM((2, n, rows, size), jnp.bfloat16),
            pltpu.VMEM((size // 2, rows), jnp.float32),
            pltpu.VMEM((rows, size), jnp.float32),
            pltpu.VMEM((rows, size), jnp.float32),
            pltpu.VMEM((length // PAGE, size), jnp.float32),
            pltpu.VMEM((length // PAGE, size), jnp.float32),
            pltpu.SemaphoreType.DMA((3,)),
            pltpu.SemaphoreType.DMA((4 * n + 6,)),
            pltpu.SemaphoreType.DMA((4 * n + 6,)),
            pltpu.SemaphoreType.DMA((2 * n,)),
            pltpu.SemaphoreType.DMA((2 * n,)),
        ],
        compiler_params=pltpu.CompilerParams(
            collective_id=0, has_side_effects=True, vmem_limit_bytes=36 << 20
        ),
        name="exchange",
    )(fresh_keys.reshape(plain), fresh_values.reshape(plain), turn_angle.T)
    keys, values, high, low = out
    return (
        keys[None, None],
        values.reshape(1, length, 1, size),
        high.reshape(1, length // PAGE, 1, size),
        low.reshape(1, length // PAGE, 1, size),
    )


def solution(mesh):
    placed = (
        P(None, ("block", "span"), "model", None),
        P(None, ("block", "span"), "model", None),
        P(),
    )
    return jax.shard_map(
        body,
        mesh=mesh,
        in_specs=placed,
        out_specs=(
            P(("block", "span"), "model", None, None),
            P(("block", "span"), None, "model", None),
            P(("block", "span"), None, "model", None),
            P(("block", "span"), None, "model", None),
        ),
        check_vma=False,
    )
```

```python
import functools

import jax
import jax.numpy as jnp
from jax import lax
from jax.experimental import pallas as pl
from jax.experimental.pallas import tpu as pltpu
from jax.sharding import PartitionSpec as P

PAGE = 64
MESH = pl.DeviceIdType.MESH
RING = 8
STEPS = (1, 7, 2, 6, 3, 5, 4)
PIECES = (8, 8, 1, 1)
ALONG = tuple((dz, dc) for dz in STEPS for dc in range(2))


def place(core, x, z, model):
    return ((z % 2) * 4 + x * 2 + core, z // 2, model)


def rank(core, x, z):
    return ((z % 2) * 4 + x * 2 + core) * 4 + z // 2


def exchange(
    keys, values, angle, out_keys, out_values, out_high, out_low,
    plain, turned, landed, relay, angles, cosine, sine, high, low,
    load_sem, send_sem, recv_sem, pass_send_sem, pass_recv_sem,
):
    block, span, model = (lax.axis_index(a) for a in ("block", "span", "model"))
    core, x, z = block % 2, (block // 2) % 2, span * 2 + block // 4
    me = rank(core, x, z)
    count, rows, size = plain.shape
    pages = rows // PAGE
    half = size // 2

    def remote(src, dst, ssem, rsem, to):
        return pltpu.make_async_remote_copy(
            src, dst, ssem, rsem, device_id=place(*to, model), device_id_type=MESH
        )

    def rows_of(r):
        return pl.ds(pl.multiple_of(r * rows, rows), rows)

    barrier = pltpu.get_barrier_semaphore()
    peers = [((core + dc) % 2, x, (z + dz) % RING) for dz, dc in ALONG]
    mate = (1 - core, x, z)
    across = [(c, 1 - x, z) for c in (core, 1 - core)]
    for to in peers + [mate] + across:
        pl.semaphore_signal(barrier, inc=1, device_id=place(*to, model), device_id_type=MESH)

    get_angle = pltpu.make_async_copy(angle.at[:, rows_of(me)], angles, load_sem.at[0])
    get_angle.start()
    get_keys = pltpu.make_async_copy(keys, plain, load_sem.at[1])
    get_keys.start()
    put_own = pltpu.make_async_copy(values.at[me], out_values.at[rows_of(me)], load_sem.at[2])
    put_own.start()

    n = len(ALONG)
    def along(kind, i):
        to = peers[i]
        c2, _, z2 = to
        final = rank(c2, 1 - x if kind < 2 else x, z2)
        src = (values if kind in (0, 3) else turned).at[final]
        if kind < 2:
            dst = relay.at[kind, i]
        elif kind == 2:
            dst = landed.at[me]
        else:
            dst = out_values.at[rows_of(me)]
        return remote(src, dst, send_sem.at[kind * n + i], recv_sem.at[kind * n + i], to)

    def beside(i, what):
        to = ([mate] + across)[i]
        at = 4 * n + what * 3 + i
        src = (values if what == 0 else turned).at[rank(*to)]
        dst = out_values.at[rows_of(me)] if what == 0 else landed.at[me]
        return remote(src, dst, send_sem.at[at], recv_sem.at[at], to)

    def passed(kind, i):
        dz, dc = ALONG[i]
        origin = rank((core - dc) % 2, x, (z - dz) % RING)
        dst = out_values.at[rows_of(origin)] if kind == 0 else landed.at[origin]
        return remote(
            relay.at[kind, i], dst, pass_send_sem.at[kind * n + i], pass_recv_sem.at[kind * n + i],
            across[0],
        )

    get_angle.wait()
    a = angles[...]
    ca, sa = jnp.cos(a), jnp.sin(a)
    cosine[...] = jnp.concatenate([ca, ca], axis=0).T
    sine[...] = jnp.concatenate([-sa, sa], axis=0).T

    pl.semaphore_wait(barrier, n + 3)
    for i in range(n):
        along(0, i).start()
    for i in range(3):
        beside(i, 0).start()

    get_keys.wait()
    part = 128

    def turn(j, _):
        s = j // (rows // part)
        r = pl.ds(pl.multiple_of((j % (rows // part)) * part, part), part)
        v = plain[s, r, :].astype(jnp.float32)
        w = v * cosine[r, :] + pltpu.roll(v, half, 1) * sine[r, :]
        turned[s, r, :] = w.astype(jnp.bfloat16)
        return 0

    lax.fori_loop(0, count * (rows // part), turn, 0)

    def finish(ref, s, origin):
        v = ref[s]
        out_keys[:, rows_of(origin)] = v.T
        g = v.astype(jnp.float32).reshape(pages, PAGE, size)
        at = pl.ds(pl.multiple_of(origin * pages, pages), pages)
        high[at, :] = jnp.max(g, axis=1)
        low[at, :] = jnp.min(g, axis=1)

    finish(turned, me, me)
    for kind in (1, 2):
        for i in range(n):
            along(kind, i).start()
    for i in range(3):
        beside(i, 1).start()
    for i in range(n):
        along(3, i).start()

    for kind in (0, 1):
        for i in range(n):
            along(kind, i).wait_recv()
            passed(kind, i).start()

    def origin_of(i, col):
        dz, dc = ALONG[i]
        return rank((core - dc) % 2, col, (z - dz) % RING)

    for i in range(3):
        beside(i, 1).wait_recv()
        finish(landed, rank(*([mate] + across)[i]), rank(*([mate] + across)[i]))
    for i in range(n):
        along(2, i).wait_recv()
        o = origin_of(i, x)
        finish(landed, o, o)
    for i in range(n):
        passed(1, i).wait_recv()
        o = origin_of(i, 1 - x)
        finish(landed, o, o)
    out_high[...] = high[...].astype(jnp.bfloat16)
    out_low[...] = low[...].astype(jnp.bfloat16)

    put_own.wait()
    for i in range(3):
        beside(i, 0).wait_recv()
    for i in range(n):
        passed(0, i).wait_recv()
    for i in range(n):
        along(3, i).wait_recv()
    for kind in range(4):
        for i in range(n):
            along(kind, i).wait_send()
    for what in range(2):
        for i in range(3):
            beside(i, what).wait_send()
    for kind in range(2):
        for i in range(n):
            passed(kind, i).wait_send()


def store(*refs):
    n = len(PIECES)
    sources, targets, sem = refs[:n], refs[n : 2 * n], refs[2 * n]
    copies = []
    for src, dst, pieces in zip(sources, targets, PIECES):
        rows = src.shape[0] // pieces
        for p in range(pieces):
            at = pl.ds(p * rows, rows)
            copies.append(
                pltpu.make_async_copy(src.at[at], dst.at[at], sem.at[len(copies)])
            )
    for c in copies:
        c.start()
    for c in copies:
        c.wait()


def body(fresh_keys, fresh_values, turn_angle):
    count, rows, _, size = fresh_keys.shape
    length = count * rows
    n = len(ALONG)
    plain = (count, rows, size)
    vmem = pl.BlockSpec(memory_space=pltpu.VMEM)
    hbm = pl.BlockSpec(memory_space=pltpu.HBM)
    out = pl.pallas_call(
        exchange,
        out_shape=[
            jax.ShapeDtypeStruct((size, length), jnp.bfloat16),
            jax.ShapeDtypeStruct((length, size), jnp.bfloat16),
            jax.ShapeDtypeStruct((length // PAGE, size), jnp.bfloat16),
            jax.ShapeDtypeStruct((length // PAGE, size), jnp.bfloat16),
        ],
        in_specs=[hbm] * 3,
        out_specs=[vmem] * 4,
        scratch_shapes=[
            pltpu.VMEM(plain, jnp.bfloat16),
            pltpu.VMEM(plain, jnp.bfloat16),
            pltpu.VMEM(plain, jnp.bfloat16),
            pltpu.VMEM((2, n, rows, size), jnp.bfloat16),
            pltpu.VMEM((size // 2, rows), jnp.float32),
            pltpu.VMEM((rows, size), jnp.float32),
            pltpu.VMEM((rows, size), jnp.float32),
            pltpu.VMEM((length // PAGE, size), jnp.float32),
            pltpu.VMEM((length // PAGE, size), jnp.float32),
            pltpu.SemaphoreType.DMA((3,)),
            pltpu.SemaphoreType.DMA((4 * n + 6,)),
            pltpu.SemaphoreType.DMA((4 * n + 6,)),
            pltpu.SemaphoreType.DMA((2 * n,)),
            pltpu.SemaphoreType.DMA((2 * n,)),
        ],
        compiler_params=pltpu.CompilerParams(
            collective_id=0, has_side_effects=True, vmem_limit_bytes=44 << 20
        ),
        name="exchange",
    )(fresh_keys.reshape(plain), fresh_values.reshape(plain), turn_angle.T)
    keys, values, high, low = pl.pallas_call(
        store,
        out_shape=[jax.ShapeDtypeStruct(o.shape, o.dtype) for o in out],
        in_specs=[vmem] * 4,
        out_specs=[hbm] * 4,
        scratch_shapes=[pltpu.SemaphoreType.DMA((sum(PIECES),))],
        compiler_params=pltpu.CompilerParams(vmem_limit_bytes=1 << 20),
        name="store",
    )(*out)
    return (
        keys[None, None],
        values.reshape(1, length, 1, size),
        high.reshape(1, length // PAGE, 1, size),
        low.reshape(1, length // PAGE, 1, size),
    )


def solution(mesh):
    placed = (
        P(None, ("block", "span"), "model", None),
        P(None, ("block", "span"), "model", None),
        P(),
    )
    return jax.shard_map(
        body,
        mesh=mesh,
        in_specs=placed,
        out_specs=(
            P(("block", "span"), "model", None, None),
            P(("block", "span"), None, "model", None),
            P(("block", "span"), None, "model", None),
            P(("block", "span"), None, "model", None),
        ),
        check_vma=False,
    )
```

```python
import functools

import jax
import jax.numpy as jnp
from jax import lax
from jax.experimental import pallas as pl
from jax.experimental.pallas import tpu as pltpu
from jax.sharding import PartitionSpec as P

PAGE = 64
MESH = pl.DeviceIdType.MESH
RING = 8
STEPS = (1, 7, 2, 6, 3, 5, 4)
PIECES = (8, 8, 1, 1)
ORDERS = (None, (3, 5, 1, 7, 4, 2, 6), (3, 5, 1, 7, 4, 2, 6), (3, 5, 1, 7, 4, 2, 6))
LAST = tuple(range(7))
ALONG = tuple((dz, dc) for dz in STEPS for dc in range(2))


def place(core, x, z, model):
    return ((z % 2) * 4 + x * 2 + core, z // 2, model)


def rank(core, x, z):
    return ((z % 2) * 4 + x * 2 + core) * 4 + z // 2


def exchange(
    keys, values, angle, out_keys, out_values, out_high, out_low,
    plain, turned, landed, relay, angles, cosine, sine, high, low,
    load_sem, send_sem, recv_sem, pass_send_sem, pass_recv_sem, last_sem, known,
):
    block, span, model = (lax.axis_index(a) for a in ("block", "span", "model"))
    core, x, z = block % 2, (block // 2) % 2, span * 2 + block // 4
    me = rank(core, x, z)
    count, rows, size = plain.shape
    pages = rows // PAGE
    half = size // 2

    def remote(src, dst, ssem, rsem, to):
        return pltpu.make_async_remote_copy(
            src, dst, ssem, rsem, device_id=place(*to, model), device_id_type=MESH
        )

    def rows_of(r):
        return pl.ds(pl.multiple_of(r * rows, rows), rows)

    peers = [((core + dc) % 2, x, (z + dz) % RING) for dz, dc in ALONG]
    mate = (1 - core, x, z)
    across = [(c, 1 - x, z) for c in (core, 1 - core)]
    ahead, behind = (core, x, (z + 1) % RING), (core, x, (z + RING - 1) % RING)

    def signal(sem, to):
        pl.semaphore_signal(sem, inc=1, device_id=place(*to, model), device_id_type=MESH)

    barrier = pltpu.get_barrier_semaphore()
    near = [to for to, (dz, _) in zip(peers, ALONG) if dz in (1, RING - 1)]
    for to in near + [mate] + across:
        signal(barrier, to)

    get_angle = pltpu.make_async_copy(angle.at[:, rows_of(me)], angles, load_sem.at[0])
    get_angle.start()
    get_keys = pltpu.make_async_copy(keys, plain, load_sem.at[1])
    get_keys.start()
    put_own = pltpu.make_async_copy(values.at[me], out_values.at[rows_of(me)], load_sem.at[2])
    put_own.start()

    n = len(ALONG)

    def order(kind):
        return [ALONG.index((dz, dc)) for dz in ORDERS[kind] for dc in range(2)]

    def along(kind, i):
        to = peers[i]
        c2, _, z2 = to
        final = rank(c2, 1 - x if kind < 2 else x, z2)
        src = (values if kind in (0, 3) else turned).at[final]
        if kind < 2:
            dst = relay.at[kind, i]
        elif kind == 2:
            dst = landed.at[me]
        else:
            dst = out_values.at[rows_of(me)]
        return remote(src, dst, send_sem.at[kind * n + i], recv_sem.at[kind * n + i], to)

    def last(j, dc, receiving=False):
        at = 3 * n
        if receiving:
            dz, dc = ALONG[j]
            to, owner = mate, ((z - dz) % RING) * 2 + (core - dc) % 2
        else:
            c2, z2 = (core + dc) % 2, j + jnp.where(z <= j, 1, 0)
            to, owner = (c2, x, z2), z * 2 + core
        return remote(
            values.at[rank(*to)], out_values.at[rows_of(me)],
            send_sem.at[at + j * (1 if receiving else 2) + (0 if receiving else dc)], last_sem.at[owner], to,
        )

    def beside(i, what):
        to = ([mate] + across)[i]
        at = 4 * n + what * 3 + i
        src = (values if what == 0 else turned).at[rank(*to)]
        dst = out_values.at[rows_of(me)] if what == 0 else landed.at[me]
        return remote(src, dst, send_sem.at[at], recv_sem.at[at], to)

    def passed(kind, i):
        dz, dc = ALONG[i]
        origin = rank((core - dc) % 2, x, (z - dz) % RING)
        dst = out_values.at[rows_of(origin)] if kind == 0 else landed.at[origin]
        return remote(
            relay.at[kind, i], dst, pass_send_sem.at[kind * n + i], pass_recv_sem.at[kind * n + i],
            across[0],
        )

    pl.semaphore_wait(barrier, len(near) + 3)
    for i in range(3):
        beside(i, 0).start()
    for step in range(1, RING // 2 + 1):
        for i, (dz, _) in enumerate(ALONG):
            if dz in (step, RING - step):
                along(0, i).start()
        if step < RING // 2:
            signal(known.at[step - 1, 0], ahead)
            if step < RING // 2 - 1:
                signal(known.at[step - 1, 1], behind)
            pl.semaphore_wait(known.at[step - 1, 0], 1)
            if step < RING // 2 - 1:
                pl.semaphore_wait(known.at[step - 1, 1], 1)

    get_angle.wait()
    a = angles[...]
    ca, sa = jnp.cos(a), jnp.sin(a)
    cosine[...] = jnp.concatenate([ca, ca], axis=0).T
    sine[...] = jnp.concatenate([-sa, sa], axis=0).T

    get_keys.wait()
    part = 128

    def turn(j, _):
        s = j // (rows // part)
        r = pl.ds(pl.multiple_of((j % (rows // part)) * part, part), part)
        v = plain[s, r, :].astype(jnp.float32)
        w = v * cosine[r, :] + pltpu.roll(v, half, 1) * sine[r, :]
        turned[s, r, :] = w.astype(jnp.bfloat16)
        return 0

    lax.fori_loop(0, count * (rows // part), turn, 0)

    def finish(ref, s, origin):
        v = ref[s]
        out_keys[:, rows_of(origin)] = v.T
        g = v.astype(jnp.float32).reshape(pages, PAGE, size)
        at = pl.ds(pl.multiple_of(origin * pages, pages), pages)
        high[at, :] = jnp.max(g, axis=1)
        low[at, :] = jnp.min(g, axis=1)

    finish(turned, me, me)
    for kind in (1, 2, 3):
        if kind == 3:
            for j in LAST:
                for dc in range(2):
                    last(j, dc).start()
            break
        for i in order(kind):
            along(kind, i).start()
        if kind == 2:
            for i in range(3):
                beside(i, 1).start()

    for kind in (0, 1):
        for i in range(n):
            along(kind, i).wait_recv()
            passed(kind, i).start()

    def origin_of(i, col):
        dz, dc = ALONG[i]
        return rank((core - dc) % 2, col, (z - dz) % RING)

    for i in range(3):
        beside(i, 1).wait_recv()
        finish(landed, rank(*([mate] + across)[i]), rank(*([mate] + across)[i]))
    for i in range(n):
        along(2, i).wait_recv()
        o = origin_of(i, x)
        finish(landed, o, o)
    for i in range(n):
        passed(1, i).wait_recv()
        o = origin_of(i, 1 - x)
        finish(landed, o, o)
    out_high[...] = high[...].astype(jnp.bfloat16)
    out_low[...] = low[...].astype(jnp.bfloat16)

    put_own.wait()
    for i in range(3):
        beside(i, 0).wait_recv()
    for i in range(n):
        passed(0, i).wait_recv()
    for i in range(n):
        last(i, 0, True).wait_recv()
    for kind in range(3):
        for i in range(n):
            along(kind, i).wait_send()
    for j in range(RING - 1):
        for dc in range(2):
            last(j, dc).wait_send()
    for what in range(2):
        for i in range(3):
            beside(i, what).wait_send()
    for kind in range(2):
        for i in range(n):
            passed(kind, i).wait_send()


def store(*refs):
    n = len(PIECES)
    sources, targets, sem = refs[:n], refs[n : 2 * n], refs[2 * n]
    copies = []
    for src, dst, pieces in zip(sources, targets, PIECES):
        rows = src.shape[0] // pieces
        for p in range(pieces):
            at = pl.ds(p * rows, rows)
            copies.append(
                pltpu.make_async_copy(src.at[at], dst.at[at], sem.at[len(copies)])
            )
    for c in copies:
        c.start()
    for c in copies:
        c.wait()


def body(fresh_keys, fresh_values, turn_angle):
    count, rows, _, size = fresh_keys.shape
    length = count * rows
    n = len(ALONG)
    plain = (count, rows, size)
    vmem = pl.BlockSpec(memory_space=pltpu.VMEM)
    hbm = pl.BlockSpec(memory_space=pltpu.HBM)
    out = pl.pallas_call(
        exchange,
        out_shape=[
            jax.ShapeDtypeStruct((size, length), jnp.bfloat16),
            jax.ShapeDtypeStruct((length, size), jnp.bfloat16),
            jax.ShapeDtypeStruct((length // PAGE, size), jnp.bfloat16),
            jax.ShapeDtypeStruct((length // PAGE, size), jnp.bfloat16),
        ],
        in_specs=[hbm] * 3,
        out_specs=[vmem] * 4,
        scratch_shapes=[
            pltpu.VMEM(plain, jnp.bfloat16),
            pltpu.VMEM(plain, jnp.bfloat16),
            pltpu.VMEM(plain, jnp.bfloat16),
            pltpu.VMEM((2, n, rows, size), jnp.bfloat16),
            pltpu.VMEM((size // 2, rows), jnp.float32),
            pltpu.VMEM((rows, size), jnp.float32),
            pltpu.VMEM((rows, size), jnp.float32),
            pltpu.VMEM((length // PAGE, size), jnp.float32),
            pltpu.VMEM((length // PAGE, size), jnp.float32),
            pltpu.SemaphoreType.DMA((3,)),
            pltpu.SemaphoreType.DMA((4 * n + 6,)),
            pltpu.SemaphoreType.DMA((4 * n + 6,)),
            pltpu.SemaphoreType.DMA((2 * n,)),
            pltpu.SemaphoreType.DMA((2 * n,)),
            pltpu.SemaphoreType.DMA((2 * RING,)),
            pltpu.SemaphoreType.REGULAR((RING // 2 - 1, 2)),
        ],
        compiler_params=pltpu.CompilerParams(
            collective_id=0, has_side_effects=True, vmem_limit_bytes=44 << 20
        ),
        name="exchange",
    )(fresh_keys.reshape(plain), fresh_values.reshape(plain), turn_angle.T)
    keys, values, high, low = pl.pallas_call(
        store,
        out_shape=[jax.ShapeDtypeStruct(o.shape, o.dtype) for o in out],
        in_specs=[vmem] * 4,
        out_specs=[hbm] * 4,
        scratch_shapes=[pltpu.SemaphoreType.DMA((sum(PIECES),))],
        compiler_params=pltpu.CompilerParams(vmem_limit_bytes=1 << 20),
        name="store",
    )(*out)
    return (
        keys[None, None],
        values.reshape(1, length, 1, size),
        high.reshape(1, length // PAGE, 1, size),
        low.reshape(1, length // PAGE, 1, size),
    )


def solution(mesh):
    placed = (
        P(None, ("block", "span"), "model", None),
        P(None, ("block", "span"), "model", None),
        P(),
    )
    return jax.shard_map(
        body,
        mesh=mesh,
        in_specs=placed,
        out_specs=(
            P(("block", "span"), "model", None, None),
            P(("block", "span"), None, "model", None),
            P(("block", "span"), None, "model", None),
            P(("block", "span"), None, "model", None),
        ),
        check_vma=False,
    )
```

```python
import functools

import jax
import jax.numpy as jnp
from jax import lax
from jax.experimental import pallas as pl
from jax.experimental.pallas import tpu as pltpu
from jax.sharding import PartitionSpec as P

PAGE = 64
MESH = pl.DeviceIdType.MESH
RING = 8
PIECES = (4, 4, 1, 1)
EARLY = (1, 7, 2, 6, 3, 5, 4)
LATER = (3, 5, 1, 7, 4, 2, 6)
FINAL = (
    (7, 5, 6, 4, 3, 2, 1),
    (0, 4, 5, 7, 6, 2, 3),
    (0, 1, 6, 7, 5, 4, 3),
    (0, 1, 2, 7, 6, 5, 4),
    (1, 0, 2, 7, 3, 6, 5),
    (0, 1, 7, 2, 6, 3, 4),
    (0, 3, 1, 4, 2, 5, 7),
    (0, 3, 1, 4, 2, 5, 6),
)
ALONG = tuple((dz, dc) for dz in EARLY for dc in range(2))
PART = 128


def place(core, x, z, model):
    return ((z % 2) * 4 + x * 2 + core, z // 2, model)


def rank(core, x, z):
    return ((z % 2) * 4 + x * 2 + core) * 4 + z // 2


def exchange(
    keys, values, angle, out_keys, out_values, out_high, out_low,
    plain, turned, landed, relay, angles, cosine, sine, high, low,
    load_sem, send_sem, recv_sem, pass_send_sem, pass_recv_sem, last_send_sem, last_recv_sem,
    inside, known, staged, stage_sem,
):
    block, span, model = (lax.axis_index(a) for a in ("block", "span", "model"))
    core, x, z = block % 2, (block // 2) % 2, span * 2 + block // 4
    me = rank(core, x, z)
    count, rows, size = plain.shape
    pages = rows // PAGE
    half = size // 2
    n = len(ALONG)

    def remote(src, dst, ssem, rsem, to):
        return pltpu.make_async_remote_copy(
            src, dst, ssem, rsem, device_id=place(*to, model), device_id_type=MESH
        )

    def signal(sem, *devices):
        for to in devices:
            pl.semaphore_signal(sem, inc=1, device_id=place(*to, model), device_id_type=MESH)

    def rows_of(r):
        return pl.ds(pl.multiple_of(r * rows, rows), rows)

    peers = [((core + dc) % 2, x, (z + dz) % RING) for dz, dc in ALONG]
    mate = (1 - core, x, z)
    across = [(c, 1 - x, z) for c in (core, 1 - core)]
    ahead = [(c, x, (z + 1) % RING) for c in (core, 1 - core)]
    behind = [(c, x, (z + RING - 1) % RING) for c in (core, 1 - core)]

    def sends_to(dz):
        return [i for i, (d, _) in enumerate(ALONG) if d == dz]

    first_of_ahead = z <= 5
    first_of_behind = (z == 0) | (z == 7)
    first_of_across = x == 0
    first_of_mate = core == 1
    barrier = pltpu.get_barrier_semaphore()

    @pl.when(first_of_ahead)
    def _():
        signal(barrier, *ahead)

    @pl.when(first_of_behind)
    def _():
        signal(barrier, *behind)

    @pl.when(first_of_across)
    def _():
        signal(barrier, *across)

    @pl.when(first_of_mate)
    def _():
        signal(barrier, mate)

    def stage(side, i):
        c2, _, z2 = peers[i]
        return pltpu.make_async_copy(
            values.at[rank(c2, 1 - x, z2)], staged.at[side, ALONG[i][1]], stage_sem.at[side, ALONG[i][1]]
        )

    @pl.when(first_of_ahead)
    def _():
        for i in sends_to(1):
            stage(0, i).start()

    @pl.when(first_of_behind)
    def _():
        for i in sends_to(RING - 1):
            stage(1, i).start()

    get_angle = pltpu.make_async_copy(angle.at[:, rows_of(me)], angles, load_sem.at[0])
    get_angle.start()
    get_keys = pltpu.make_async_copy(keys, plain, load_sem.at[1])
    get_keys.start()
    put_own = pltpu.make_async_copy(values.at[me], out_values.at[rows_of(me)], load_sem.at[2])
    put_own.start()

    def along(kind, i, src=None):
        c2, _, z2 = to = peers[i]
        final = rank(c2, 1 - x if kind < 2 else x, z2)
        if src is None:
            src = (values if kind == 0 else turned).at[final]
        dst = relay.at[kind, i] if kind < 2 else landed.at[me]
        return remote(src, dst, send_sem.at[kind * n + i], recv_sem.at[kind * n + i], to)

    def beside(what, i):
        to = ([mate] + across)[i]
        at = 3 * n + what * 3 + i
        src = (values if what == 0 else turned).at[rank(*to)]
        dst = out_values.at[rows_of(me)] if what == 0 else landed.at[me]
        return remote(src, dst, send_sem.at[at], recv_sem.at[at], to)

    def origin(i, column):
        dz, dc = ALONG[i]
        return rank((core - dc) % 2, column, (z - dz) % RING)

    def passed(kind, i):
        dst = out_values.at[rows_of(origin(i, x))] if kind == 0 else landed.at[origin(i, x)]
        return remote(
            relay.at[kind, i], dst, pass_send_sem.at[kind * n + i], pass_recv_sem.at[kind * n + i],
            across[0],
        )


    def last(j, dc):
        to = ((core + dc) % 2, x, sum(jnp.where(z == k, t[j], 0) for k, t in enumerate(FINAL)))
        return remote(
            values.at[rank(*to)], out_values.at[rows_of(me)],
            last_send_sem.at[2 * j + dc], last_recv_sem.at[2 * z + core], to,
        )

    def last_from(i):
        dz, dc = ALONG[i]
        at = 2 * ((z - dz) % RING) + (core - dc) % 2
        src = out_values.at[rows_of(origin(i, x))]
        return remote(src, src, last_send_sem.at[0], last_recv_sem.at[at], peers[i])

    due = jnp.where(z == 6, 4, jnp.where(z == 0, 0, 2)) + 2 * x + 1 - core

    @pl.when(due > 0)
    def _():
        pl.semaphore_wait(barrier, due)

    def first_sends(dz):
        for i in sends_to(dz):
            along(0, i).start()

    def staged_sends(side, dz):
        for i in sends_to(dz):
            stage(side, i).wait()
            along(0, i, staged.at[side, ALONG[i][1]]).start()

    @pl.when(jnp.logical_not(first_of_behind))
    def _():
        first_sends(RING - 1)
        signal(inside.at[0], *behind)

    @pl.when(jnp.logical_not(first_of_ahead))
    def _():
        first_sends(1)
        signal(inside.at[1], *ahead)

    @pl.when(jnp.logical_not(first_of_across))
    def _():
        signal(inside.at[2], *across)

    @pl.when(jnp.logical_not(first_of_mate))
    def _():
        signal(inside.at[3], mate)

    @pl.when(first_of_ahead)
    def _():
        pl.semaphore_wait(inside.at[0], 2)
        staged_sends(0, 1)

    @pl.when(first_of_behind)
    def _():
        pl.semaphore_wait(inside.at[1], 2)
        staged_sends(1, RING - 1)

    far = RING // 2
    for step in range(1, far):
        signal(known.at[step - 1, 0], ahead[0])
        if step < far - 1:
            signal(known.at[step - 1, 1], behind[0])
        pl.semaphore_wait(known.at[step - 1, 0], 1)
        if step < far - 1:
            pl.semaphore_wait(known.at[step - 1, 1], 1)
        for dz in sorted({step + 1, RING - step - 1}):
            first_sends(dz)

    @pl.when(first_of_across)
    def _():
        pl.semaphore_wait(inside.at[2], 2)

    @pl.when(first_of_mate)
    def _():
        pl.semaphore_wait(inside.at[3], 1)

    for i in range(3):
        beside(0, i).start()

    get_angle.wait()
    a = angles[...]
    ca, sa = jnp.cos(a), jnp.sin(a)
    cosine[...] = jnp.concatenate([ca, ca], axis=0).T
    sine[...] = jnp.concatenate([-sa, sa], axis=0).T
    get_keys.wait()

    def turn(j, _):
        s = j // (rows // PART)
        r = pl.ds(pl.multiple_of((j % (rows // PART)) * PART, PART), PART)
        v = plain[s, r, :].astype(jnp.float32)
        w = v * cosine[r, :] + pltpu.roll(v, half, 1) * sine[r, :]
        turned[s, r, :] = w.astype(jnp.bfloat16)
        return 0

    lax.fori_loop(0, count * (rows // PART), turn, 0)

    def finish(ref, o):
        v = ref[o]
        out_keys[:, rows_of(o)] = v.T
        g = v.astype(jnp.float32).reshape(pages, PAGE, size)
        at = pl.ds(pl.multiple_of(o * pages, pages), pages)
        high[at, :] = jnp.max(g, axis=1)
        low[at, :] = jnp.min(g, axis=1)

    finish(turned, me)
    for kind in (1, 2):
        for dz in LATER:
            for dc in range(2):
                along(kind, ALONG.index((dz, dc))).start()
    for i in range(3):
        beside(1, i).start()
    for j in range(RING - 1):
        for dc in range(2):
            last(j, dc).start()

    for kind in (0, 1):
        for i in range(n):
            along(kind, i).wait_recv()
            passed(kind, i).start()
    for i in range(3):
        beside(1, i).wait_recv()
        finish(landed, rank(*([mate] + across)[i]))
    for i in range(n):
        along(2, i).wait_recv()
        finish(landed, origin(i, x))
    for i in range(n):
        passed(1, i).wait_recv()
        finish(landed, origin(i, 1 - x))
    out_high[...] = high[...].astype(jnp.bfloat16)
    out_low[...] = low[...].astype(jnp.bfloat16)

    put_own.wait()
    for i in range(3):
        beside(0, i).wait_recv()
        for what in range(2):
            beside(what, i).wait_send()
    for i in range(n):
        passed(0, i).wait_recv()
        for kind in range(2):
            passed(kind, i).wait_send()
        for kind in range(3):
            along(kind, i).wait_send()
    for i in range(n):
        last_from(i).wait_recv()
    for j in range(RING - 1):
        for dc in range(2):
            last(j, dc).wait_send()


def store(*refs):
    n = len(PIECES)
    sources, targets, sem = refs[:n], refs[n : 2 * n], refs[2 * n]
    copies = []
    for src, dst, pieces in zip(sources, targets, PIECES):
        rows = src.shape[0] // pieces
        for p in range(pieces):
            at = pl.ds(p * rows, rows)
            copies.append(
                pltpu.make_async_copy(src.at[at], dst.at[at], sem.at[len(copies)])
            )
    for c in copies:
        c.start()
    for c in copies:
        c.wait()


def body(fresh_keys, fresh_values, turn_angle):
    count, rows, _, size = fresh_keys.shape
    length = count * rows
    n = len(ALONG)
    plain = (count, rows, size)
    vmem = pl.BlockSpec(memory_space=pltpu.VMEM)
    hbm = pl.BlockSpec(memory_space=pl.ANY)
    dma = pltpu.SemaphoreType.DMA
    out = pl.pallas_call(
        exchange,
        out_shape=[
            jax.ShapeDtypeStruct((size, length), jnp.bfloat16),
            jax.ShapeDtypeStruct((length, size), jnp.bfloat16),
            jax.ShapeDtypeStruct((length // PAGE, size), jnp.bfloat16),
            jax.ShapeDtypeStruct((length // PAGE, size), jnp.bfloat16),
        ],
        in_specs=[hbm] * 3,
        out_specs=[vmem] * 4,
        scratch_shapes=[
            pltpu.VMEM(plain, jnp.bfloat16),
            pltpu.VMEM(plain, jnp.bfloat16),
            pltpu.VMEM(plain, jnp.bfloat16),
            pltpu.VMEM((2, n, rows, size), jnp.bfloat16),
            pltpu.VMEM((size // 2, rows), jnp.float32),
            pltpu.VMEM((rows, size), jnp.float32),
            pltpu.VMEM((rows, size), jnp.float32),
            pltpu.VMEM((length // PAGE, size), jnp.float32),
            pltpu.VMEM((length // PAGE, size), jnp.float32),
            dma((3,)),
            dma((3 * n + 6,)),
            dma((3 * n + 6,)),
            dma((2 * n,)),
            dma((2 * n,)),
            dma((n,)),
            dma((2 * RING,)),
            pltpu.SemaphoreType.REGULAR((4,)),
            pltpu.SemaphoreType.REGULAR((RING // 2 - 1, 2)),
            pltpu.VMEM((2, 2, rows, size), jnp.bfloat16),
            dma((2, 2)),
        ],
        compiler_params=pltpu.CompilerParams(
            collective_id=0, has_side_effects=True, vmem_limit_bytes=44 << 20
        ),
        name="exchange",
    )(fresh_keys.reshape(plain), fresh_values.reshape(plain), turn_angle.T)
    keys, values, high, low = pl.pallas_call(
        store,
        out_shape=[jax.ShapeDtypeStruct(o.shape, o.dtype) for o in out],
        in_specs=[vmem] * 4,
        out_specs=[hbm] * 4,
        scratch_shapes=[dma((sum(PIECES),))],
        compiler_params=pltpu.CompilerParams(vmem_limit_bytes=1 << 20),
        name="store",
    )(*out)
    return (
        keys[None, None],
        values.reshape(1, length, 1, size),
        high.reshape(1, length // PAGE, 1, size),
        low.reshape(1, length // PAGE, 1, size),
    )


def solution(mesh):
    placed = (
        P(None, ("block", "span"), "model", None),
        P(None, ("block", "span"), "model", None),
        P(),
    )
    return jax.shard_map(
        body,
        mesh=mesh,
        in_specs=placed,
        out_specs=(
            P(("block", "span"), "model", None, None),
            P(("block", "span"), None, "model", None),
            P(("block", "span"), None, "model", None),
            P(("block", "span"), None, "model", None),
        ),
        check_vma=False,
    )
```

```python
import functools

import jax
import jax.numpy as jnp
from jax import lax
from jax.experimental import pallas as pl
from jax.experimental.pallas import tpu as pltpu
from jax.sharding import PartitionSpec as P

PAGE = 64
MESH = pl.DeviceIdType.MESH
RING = 8
PIECES = (4, 4, 1, 1)
EARLY = (1, 7, 2, 6, 3, 5, 4)
LATER = (3, 5, 1, 7, 4, 2, 6)
FINAL = (
    (7, 5, 6, 3, 2, 1),
    (0, 4, 7, 6, 2, 3),
    (0, 1, 7, 5, 4, 3),
    (0, 1, 2, 6, 5, 4),
    (1, 2, 7, 3, 6, 5),
    (0, 7, 2, 6, 3, 4),
    (0, 3, 1, 4, 5, 7),
    (0, 1, 4, 2, 5, 6),
)
ALONG = tuple((dz, dc) for dz in EARLY for dc in range(2))
DETOUR = 256
PART = 128


def place(core, x, z, model):
    return ((z % 2) * 4 + x * 2 + core, z // 2, model)


def rank(core, x, z):
    return ((z % 2) * 4 + x * 2 + core) * 4 + z // 2


def exchange(
    keys, values, angle, out_keys, out_values, out_high, out_low,
    plain, turned, landed, relay, angles, cosine, sine, high, low,
    load_sem, send_sem, recv_sem, pass_send_sem, pass_recv_sem, last_send_sem, last_recv_sem,
    inside, known, staged, stage_sem, detour, far_send_sem, far_recv_sem,
):
    block, span, model = (lax.axis_index(a) for a in ("block", "span", "model"))
    core, x, z = block % 2, (block // 2) % 2, span * 2 + block // 4
    me = rank(core, x, z)
    count, rows, size = plain.shape
    pages = rows // PAGE
    half = size // 2
    n = len(ALONG)

    def remote(src, dst, ssem, rsem, to):
        return pltpu.make_async_remote_copy(
            src, dst, ssem, rsem, device_id=place(*to, model), device_id_type=MESH
        )

    def signal(sem, *devices):
        for to in devices:
            pl.semaphore_signal(sem, inc=1, device_id=place(*to, model), device_id_type=MESH)

    def rows_of(r):
        return pl.ds(pl.multiple_of(r * rows, rows), rows)

    peers = [((core + dc) % 2, x, (z + dz) % RING) for dz, dc in ALONG]
    mate = (1 - core, x, z)
    across = [(c, 1 - x, z) for c in (core, 1 - core)]
    ahead = [(c, x, (z + 1) % RING) for c in (core, 1 - core)]
    behind = [(c, x, (z + RING - 1) % RING) for c in (core, 1 - core)]

    def sends_to(dz):
        return [i for i, (d, _) in enumerate(ALONG) if d == dz]

    first_of_ahead = z <= 5
    first_of_behind = (z == 0) | (z == 7)
    first_of_across = x == 0
    first_of_mate = core == 1
    barrier = pltpu.get_barrier_semaphore()

    @pl.when(first_of_ahead)
    def _():
        signal(barrier, *ahead)

    @pl.when(first_of_behind)
    def _():
        signal(barrier, *behind)

    @pl.when(first_of_across)
    def _():
        signal(barrier, *across)

    @pl.when(first_of_mate)
    def _():
        signal(barrier, mate)

    def stage(side, i):
        c2, _, z2 = peers[i]
        return pltpu.make_async_copy(
            values.at[rank(c2, 1 - x, z2)], staged.at[side, ALONG[i][1]], stage_sem.at[side, ALONG[i][1]]
        )

    @pl.when(first_of_ahead)
    def _():
        for i in sends_to(1):
            stage(0, i).start()

    @pl.when(first_of_behind)
    def _():
        for i in sends_to(RING - 1):
            stage(1, i).start()

    get_angle = pltpu.make_async_copy(angle.at[:, rows_of(me)], angles, load_sem.at[0])
    get_angle.start()
    get_keys = pltpu.make_async_copy(keys, plain, load_sem.at[1])
    get_keys.start()
    put_own = pltpu.make_async_copy(values.at[me], out_values.at[rows_of(me)], load_sem.at[2])
    put_own.start()

    def along(kind, i, src=None):
        c2, _, z2 = to = peers[i]
        final = rank(c2, 1 - x if kind < 2 else x, z2)
        if src is None:
            src = (values if kind == 0 else turned).at[final]
        dst = relay.at[kind, i] if kind < 2 else landed.at[me]
        return remote(src, dst, send_sem.at[kind * n + i], recv_sem.at[kind * n + i], to)

    def beside(what, i):
        to = ([mate] + across)[i]
        at = 3 * n + what * 3 + i
        src = (values if what == 0 else turned).at[rank(*to)]
        dst = out_values.at[rows_of(me)] if what == 0 else landed.at[me]
        return remote(src, dst, send_sem.at[at], recv_sem.at[at], to)

    def origin(i, column):
        dz, dc = ALONG[i]
        return rank((core - dc) % 2, column, (z - dz) % RING)

    def passed(kind, i):
        dst = out_values.at[rows_of(origin(i, x))] if kind == 0 else landed.at[origin(i, x)]
        return remote(
            relay.at[kind, i], dst, pass_send_sem.at[kind * n + i], pass_recv_sem.at[kind * n + i],
            across[0],
        )


    def last(j, dc):
        to = ((core + dc) % 2, x, sum(jnp.where(z == k, t[j], 0) for k, t in enumerate(FINAL)))
        return remote(
            values.at[rank(*to)], out_values.at[rows_of(me)],
            last_send_sem.at[2 * j + dc], last_recv_sem.at[2 * z + core], to,
        )

    opposite = (z + RING // 2) % RING
    goes_round = (z == 1) | (z == 6)
    between = (z == 3) | (z == 4)
    front, back = pl.ds(0, rows - DETOUR), pl.ds(rows - DETOUR, DETOUR)

    def back_of(r):
        return pl.ds(pl.multiple_of(r * rows + rows - DETOUR, DETOUR), DETOUR)

    def over(part):
        to = (1 - core if part == 0 else core, x, opposite)
        src = values.at[rank(*to)]
        if part == 0:
            dst = out_values.at[rows_of(me)]
        elif part == 1:
            src, dst = src.at[front], out_values.at[pl.ds(pl.multiple_of(me * rows, rows), rows - DETOUR)]
        else:
            src, dst = src.at[back], out_values.at[back_of(me)]
        return remote(src, dst, far_send_sem.at[part], far_recv_sem.at[part], to)

    def over_from(part):
        o = rank(1 - core if part == 0 else core, x, opposite)
        if part == 0:
            src = out_values.at[rows_of(o)]
        elif part == 1:
            src = out_values.at[pl.ds(pl.multiple_of(o * rows, rows), rows - DETOUR)]
        else:
            src = out_values.at[back_of(o)]
        return remote(src, src, far_send_sem.at[part], far_recv_sem.at[part], (core, x, opposite))

    def go_round():
        final = rank(core, x, opposite)
        return remote(
            values.at[final, back], detour, far_send_sem.at[3], far_recv_sem.at[3],
            (core, x, jnp.where(z == 6, 4, 3)),
        )

    def go_on():
        o = rank(core, x, jnp.where(z == 4, 6, 1))
        return remote(
            detour, out_values.at[back_of(o)], far_send_sem.at[4], far_recv_sem.at[2],
            (core, x, jnp.where(z == 4, 2, 5)),
        )

    def last_from(i):
        dz, dc = ALONG[i]
        at = 2 * ((z - dz) % RING) + (core - dc) % 2
        src = out_values.at[rows_of(origin(i, x))]
        return remote(src, src, last_send_sem.at[0], last_recv_sem.at[at], peers[i])

    due = jnp.where(z == 6, 4, jnp.where(z == 0, 0, 2)) + 2 * x + 1 - core

    @pl.when(due > 0)
    def _():
        pl.semaphore_wait(barrier, due)

    def first_sends(dz):
        for i in sends_to(dz):
            along(0, i).start()

    def staged_sends(side, dz):
        for i in sends_to(dz):
            stage(side, i).wait()
            along(0, i, staged.at[side, ALONG[i][1]]).start()

    @pl.when(jnp.logical_not(first_of_behind))
    def _():
        first_sends(RING - 1)
        signal(inside.at[0], *behind)

    @pl.when(jnp.logical_not(first_of_ahead))
    def _():
        first_sends(1)
        signal(inside.at[1], *ahead)

    @pl.when(jnp.logical_not(first_of_across))
    def _():
        signal(inside.at[2], *across)

    @pl.when(jnp.logical_not(first_of_mate))
    def _():
        signal(inside.at[3], mate)

    @pl.when(first_of_ahead)
    def _():
        pl.semaphore_wait(inside.at[0], 2)
        staged_sends(0, 1)

    @pl.when(first_of_behind)
    def _():
        pl.semaphore_wait(inside.at[1], 2)
        staged_sends(1, RING - 1)

    far = RING // 2
    for step in range(1, far):
        signal(known.at[step - 1, 0], ahead[0])
        if step < far - 1:
            signal(known.at[step - 1, 1], behind[0])
        pl.semaphore_wait(known.at[step - 1, 0], 1)
        if step < far - 1:
            pl.semaphore_wait(known.at[step - 1, 1], 1)
        for dz in sorted({step + 1, RING - step - 1}):
            first_sends(dz)

    @pl.when(goes_round)
    def _():
        go_round().start()

    @pl.when(first_of_across)
    def _():
        pl.semaphore_wait(inside.at[2], 2)

    @pl.when(first_of_mate)
    def _():
        pl.semaphore_wait(inside.at[3], 1)

    for i in range(3):
        beside(0, i).start()

    get_angle.wait()
    a = angles[...]
    ca, sa = jnp.cos(a), jnp.sin(a)
    cosine[...] = jnp.concatenate([ca, ca], axis=0).T
    sine[...] = jnp.concatenate([-sa, sa], axis=0).T
    get_keys.wait()

    def turn(j, _):
        s = j // (rows // PART)
        r = pl.ds(pl.multiple_of((j % (rows // PART)) * PART, PART), PART)
        v = plain[s, r, :].astype(jnp.float32)
        w = v * cosine[r, :] + pltpu.roll(v, half, 1) * sine[r, :]
        turned[s, r, :] = w.astype(jnp.bfloat16)
        return 0

    lax.fori_loop(0, count * (rows // PART), turn, 0)

    def finish(ref, o):
        v = ref[o]
        out_keys[:, rows_of(o)] = v.T
        g = v.astype(jnp.float32).reshape(pages, PAGE, size)
        at = pl.ds(pl.multiple_of(o * pages, pages), pages)
        high[at, :] = jnp.max(g, axis=1)
        low[at, :] = jnp.min(g, axis=1)

    finish(turned, me)
    for kind in (1, 2):
        for dz in LATER:
            for dc in range(2):
                along(kind, ALONG.index((dz, dc))).start()
    for i in range(3):
        beside(1, i).start()
    for i in range(n):
        along(0, i).wait_recv()
        passed(0, i).start()

    @pl.when(between)
    def _():
        go_round().wait_recv()
        go_on().start()

    for part in (0, 1):
        over(part).start()

    @pl.when(jnp.logical_not(goes_round))
    def _():
        over(2).start()

    for j in range(RING - 2):
        for dc in range(2):
            last(j, dc).start()

    for i in range(n):
        along(1, i).wait_recv()
        passed(1, i).start()
    for i in range(3):
        beside(1, i).wait_recv()
        finish(landed, rank(*([mate] + across)[i]))
    for i in range(n):
        along(2, i).wait_recv()
        finish(landed, origin(i, x))
    for i in range(n):
        passed(1, i).wait_recv()
        finish(landed, origin(i, 1 - x))
    out_high[...] = high[...].astype(jnp.bfloat16)
    out_low[...] = low[...].astype(jnp.bfloat16)

    put_own.wait()
    for i in range(3):
        beside(0, i).wait_recv()
        for what in range(2):
            beside(what, i).wait_send()
    for i in range(n):
        passed(0, i).wait_recv()
        for kind in range(2):
            passed(kind, i).wait_send()
        for kind in range(3):
            along(kind, i).wait_send()
    @pl.when(goes_round)
    def _():
        go_round().wait_send()

    @pl.when(jnp.logical_not(goes_round))
    def _():
        over(2).wait_send()

    @pl.when(between)
    def _():
        go_on().wait_send()

    for part in (0, 1):
        over(part).wait_send()
    for part in (0, 1, 2):
        over_from(part).wait_recv()
    for i in range(n):
        if ALONG[i][0] != RING // 2:
            last_from(i).wait_recv()
    for j in range(RING - 2):
        for dc in range(2):
            last(j, dc).wait_send()


def store(*refs):
    n = len(PIECES)
    sources, targets, sem = refs[:n], refs[n : 2 * n], refs[2 * n]
    copies = []
    for src, dst, pieces in zip(sources, targets, PIECES):
        rows = src.shape[0] // pieces
        for p in range(pieces):
            at = pl.ds(p * rows, rows)
            copies.append(
                pltpu.make_async_copy(src.at[at], dst.at[at], sem.at[len(copies)])
            )
    for c in copies:
        c.start()
    for c in copies:
        c.wait()


def body(fresh_keys, fresh_values, turn_angle):
    count, rows, _, size = fresh_keys.shape
    length = count * rows
    n = len(ALONG)
    plain = (count, rows, size)
    vmem = pl.BlockSpec(memory_space=pltpu.VMEM)
    hbm = pl.BlockSpec(memory_space=pl.ANY)
    dma = pltpu.SemaphoreType.DMA
    out = pl.pallas_call(
        exchange,
        out_shape=[
            jax.ShapeDtypeStruct((size, length), jnp.bfloat16),
            jax.ShapeDtypeStruct((length, size), jnp.bfloat16),
            jax.ShapeDtypeStruct((length // PAGE, size), jnp.bfloat16),
            jax.ShapeDtypeStruct((length // PAGE, size), jnp.bfloat16),
        ],
        in_specs=[hbm] * 3,
        out_specs=[vmem] * 4,
        scratch_shapes=[
            pltpu.VMEM(plain, jnp.bfloat16),
            pltpu.VMEM(plain, jnp.bfloat16),
            pltpu.VMEM(plain, jnp.bfloat16),
            pltpu.VMEM((2, n, rows, size), jnp.bfloat16),
            pltpu.VMEM((size // 2, rows), jnp.float32),
            pltpu.VMEM((rows, size), jnp.float32),
            pltpu.VMEM((rows, size), jnp.float32),
            pltpu.VMEM((length // PAGE, size), jnp.float32),
            pltpu.VMEM((length // PAGE, size), jnp.float32),
            dma((3,)),
            dma((3 * n + 6,)),
            dma((3 * n + 6,)),
            dma((2 * n,)),
            dma((2 * n,)),
            dma((2 * (RING - 2),)),
            dma((2 * RING,)),
            pltpu.SemaphoreType.REGULAR((4,)),
            pltpu.SemaphoreType.REGULAR((RING // 2 - 1, 2)),
            pltpu.VMEM((2, 2, rows, size), jnp.bfloat16),
            dma((2, 2)),
            pltpu.VMEM((DETOUR, size), jnp.bfloat16),
            dma((5,)),
            dma((4,)),
        ],
        compiler_params=pltpu.CompilerParams(
            collective_id=0, has_side_effects=True, vmem_limit_bytes=44 << 20
        ),
        name="exchange",
    )(fresh_keys.reshape(plain), fresh_values.reshape(plain), turn_angle.T)
    keys, values, high, low = pl.pallas_call(
        store,
        out_shape=[jax.ShapeDtypeStruct(o.shape, o.dtype) for o in out],
        in_specs=[vmem] * 4,
        out_specs=[hbm] * 4,
        scratch_shapes=[dma((sum(PIECES),))],
        compiler_params=pltpu.CompilerParams(vmem_limit_bytes=1 << 20),
        name="store",
    )(*out)
    return (
        keys[None, None],
        values.reshape(1, length, 1, size),
        high.reshape(1, length // PAGE, 1, size),
        low.reshape(1, length // PAGE, 1, size),
    )


def solution(mesh):
    placed = (
        P(None, ("block", "span"), "model", None),
        P(None, ("block", "span"), "model", None),
        P(),
    )
    return jax.shard_map(
        body,
        mesh=mesh,
        in_specs=placed,
        out_specs=(
            P(("block", "span"), "model", None, None),
            P(("block", "span"), None, "model", None),
            P(("block", "span"), None, "model", None),
            P(("block", "span"), None, "model", None),
        ),
        check_vma=False,
    )
```

```python
import functools

import jax
import jax.numpy as jnp
from jax import lax
from jax.experimental import pallas as pl
from jax.experimental.pallas import tpu as pltpu
from jax.sharding import PartitionSpec as P

PAGE = 64
MESH = pl.DeviceIdType.MESH
RING = 8
PIECES = (4, 4, 1, 1)
EARLY = (1, 7, 2, 6, 3, 5, 4)
LATER = (3, 5, 1, 7, 4, 2, 6)
FINAL = (
    (7, 5, 6, 3, 2, 1),
    (0, 4, 7, 6, 2, 3),
    (0, 1, 7, 5, 4, 3),
    (0, 1, 2, 6, 5, 4),
    (1, 2, 7, 3, 6, 5),
    (0, 7, 2, 6, 3, 4),
    (0, 3, 1, 4, 5, 7),
    (0, 1, 4, 2, 5, 6),
)
ALONG = tuple((dz, dc) for dz in EARLY for dc in range(2))
DETOUR = 192
PART = 128


def place(core, x, z, model):
    return ((z % 2) * 4 + x * 2 + core, z // 2, model)


def rank(core, x, z):
    return ((z % 2) * 4 + x * 2 + core) * 4 + z // 2


def exchange(
    keys, values, angle, out_keys, out_values, out_high, out_low,
    plain, turned, landed, relay, angles, cosine, sine, high, low,
    load_sem, send_sem, recv_sem, pass_send_sem, pass_recv_sem, last_send_sem, last_recv_sem,
    inside, known, staged, stage_sem, detour, far_send_sem, far_recv_sem,
):
    block, span, model = (lax.axis_index(a) for a in ("block", "span", "model"))
    core, x, z = block % 2, (block // 2) % 2, span * 2 + block // 4
    me = rank(core, x, z)
    count, rows, size = plain.shape
    pages = rows // PAGE
    half = size // 2
    n = len(ALONG)

    def remote(src, dst, ssem, rsem, to):
        return pltpu.make_async_remote_copy(
            src, dst, ssem, rsem, device_id=place(*to, model), device_id_type=MESH
        )

    def signal(sem, *devices):
        for to in devices:
            pl.semaphore_signal(sem, inc=1, device_id=place(*to, model), device_id_type=MESH)

    def rows_of(r):
        return pl.ds(pl.multiple_of(r * rows, rows), rows)

    peers = [((core + dc) % 2, x, (z + dz) % RING) for dz, dc in ALONG]
    mate = (1 - core, x, z)
    across = [(c, 1 - x, z) for c in (core, 1 - core)]
    ahead = [(c, x, (z + 1) % RING) for c in (core, 1 - core)]
    behind = [(c, x, (z + RING - 1) % RING) for c in (core, 1 - core)]

    def sends_to(dz):
        return [i for i, (d, _) in enumerate(ALONG) if d == dz]

    first_of_ahead = z <= 5
    first_of_behind = (z == 0) | (z == 7)
    first_of_across = x == 0
    first_of_mate = core == 1
    barrier = pltpu.get_barrier_semaphore()

    @pl.when(first_of_ahead)
    def _():
        signal(barrier, *ahead)

    @pl.when(first_of_behind)
    def _():
        signal(barrier, *behind)

    @pl.when(first_of_across)
    def _():
        signal(barrier, *across)

    @pl.when(first_of_mate)
    def _():
        signal(barrier, mate)

    def stage(side, i):
        c2, _, z2 = peers[i]
        return pltpu.make_async_copy(
            values.at[rank(c2, 1 - x, z2)], staged.at[side, ALONG[i][1]], stage_sem.at[side, ALONG[i][1]]
        )

    @pl.when(first_of_ahead)
    def _():
        for i in sends_to(1):
            stage(0, i).start()

    @pl.when(first_of_behind)
    def _():
        for i in sends_to(RING - 1):
            stage(1, i).start()

    get_angle = pltpu.make_async_copy(angle.at[:, rows_of(me)], angles, load_sem.at[0])
    get_angle.start()
    get_keys = pltpu.make_async_copy(keys, plain, load_sem.at[1])
    get_keys.start()
    put_own = pltpu.make_async_copy(values.at[me], out_values.at[rows_of(me)], load_sem.at[2])
    put_own.start()

    def along(kind, i, src=None):
        c2, _, z2 = to = peers[i]
        final = rank(c2, 1 - x if kind < 2 else x, z2)
        if src is None:
            src = (values if kind == 0 else turned).at[final]
        dst = relay.at[kind, i] if kind < 2 else landed.at[me]
        return remote(src, dst, send_sem.at[kind * n + i], recv_sem.at[kind * n + i], to)

    def beside(what, i):
        to = ([mate] + across)[i]
        at = 3 * n + what * 3 + i
        src = (values if what == 0 else turned).at[rank(*to)]
        dst = out_values.at[rows_of(me)] if what == 0 else landed.at[me]
        return remote(src, dst, send_sem.at[at], recv_sem.at[at], to)

    def origin(i, column):
        dz, dc = ALONG[i]
        return rank((core - dc) % 2, column, (z - dz) % RING)

    def passed(kind, i):
        dst = out_values.at[rows_of(origin(i, x))] if kind == 0 else landed.at[origin(i, x)]
        return remote(
            relay.at[kind, i], dst, pass_send_sem.at[kind * n + i], pass_recv_sem.at[kind * n + i],
            across[0],
        )


    def last(j, dc):
        to = ((core + dc) % 2, x, sum(jnp.where(z == k, t[j], 0) for k, t in enumerate(FINAL)))
        return remote(
            values.at[rank(*to)], out_values.at[rows_of(me)],
            last_send_sem.at[2 * j + dc], last_recv_sem.at[2 * z + core], to,
        )

    opposite = (z + RING // 2) % RING
    goes_round = (z == 1) | (z == 6)
    between = (z == 3) | (z == 4)
    front, back = pl.ds(0, rows - DETOUR), pl.ds(rows - DETOUR, DETOUR)

    def back_of(r):
        return pl.ds(pl.multiple_of(r * rows + rows - DETOUR, 64), DETOUR)

    def over(part):
        to = (1 - core if part == 0 else core, x, opposite)
        src = values.at[rank(*to)]
        if part == 0:
            dst = out_values.at[rows_of(me)]
        elif part == 1:
            src, dst = src.at[front], out_values.at[pl.ds(pl.multiple_of(me * rows, rows), rows - DETOUR)]
        else:
            src, dst = src.at[back], out_values.at[back_of(me)]
        return remote(src, dst, far_send_sem.at[part], far_recv_sem.at[part], to)

    def over_from(part):
        o = rank(1 - core if part == 0 else core, x, opposite)
        if part == 0:
            src = out_values.at[rows_of(o)]
        elif part == 1:
            src = out_values.at[pl.ds(pl.multiple_of(o * rows, rows), rows - DETOUR)]
        else:
            src = out_values.at[back_of(o)]
        return remote(src, src, far_send_sem.at[part], far_recv_sem.at[part], (core, x, opposite))

    def go_round():
        final = rank(core, x, opposite)
        return remote(
            values.at[final, back], detour, far_send_sem.at[3], far_recv_sem.at[3],
            (core, x, jnp.where(z == 6, 4, 3)),
        )

    def go_on():
        o = rank(core, x, jnp.where(z == 4, 6, 1))
        return remote(
            detour, out_values.at[back_of(o)], far_send_sem.at[4], far_recv_sem.at[2],
            (core, x, jnp.where(z == 4, 2, 5)),
        )

    def last_from(i):
        dz, dc = ALONG[i]
        at = 2 * ((z - dz) % RING) + (core - dc) % 2
        src = out_values.at[rows_of(origin(i, x))]
        return remote(src, src, last_send_sem.at[0], last_recv_sem.at[at], peers[i])

    due = jnp.where(z == 6, 4, jnp.where(z == 0, 0, 2)) + 2 * x + 1 - core

    @pl.when(due > 0)
    def _():
        pl.semaphore_wait(barrier, due)

    def first_sends(dz):
        for i in sends_to(dz):
            along(0, i).start()

    def staged_sends(side, dz):
        for i in sends_to(dz):
            stage(side, i).wait()
            along(0, i, staged.at[side, ALONG[i][1]]).start()

    @pl.when(jnp.logical_not(first_of_behind))
    def _():
        first_sends(RING - 1)
        signal(inside.at[0], *behind)

    @pl.when(jnp.logical_not(first_of_ahead))
    def _():
        first_sends(1)
        signal(inside.at[1], *ahead)

    @pl.when(jnp.logical_not(first_of_across))
    def _():
        signal(inside.at[2], *across)

    @pl.when(jnp.logical_not(first_of_mate))
    def _():
        signal(inside.at[3], mate)

    @pl.when(first_of_ahead)
    def _():
        pl.semaphore_wait(inside.at[0], 2)
        staged_sends(0, 1)

    @pl.when(first_of_behind)
    def _():
        pl.semaphore_wait(inside.at[1], 2)
        staged_sends(1, RING - 1)

    far = RING // 2
    for step in range(1, far):
        signal(known.at[step - 1, 0], ahead[0])
        if step < far - 1:
            signal(known.at[step - 1, 1], behind[0])
        pl.semaphore_wait(known.at[step - 1, 0], 1)
        if step < far - 1:
            pl.semaphore_wait(known.at[step - 1, 1], 1)
        for dz in sorted({step + 1, RING - step - 1}):
            first_sends(dz)

    @pl.when(goes_round)
    def _():
        go_round().start()

    @pl.when(first_of_across)
    def _():
        pl.semaphore_wait(inside.at[2], 2)

    @pl.when(first_of_mate)
    def _():
        pl.semaphore_wait(inside.at[3], 1)

    for i in range(3):
        beside(0, i).start()

    get_angle.wait()
    a = angles[...]
    ca, sa = jnp.cos(a), jnp.sin(a)
    cosine[...] = jnp.concatenate([ca, ca], axis=0).T
    sine[...] = jnp.concatenate([-sa, sa], axis=0).T
    get_keys.wait()

    def turn(j, _):
        s = j // (rows // PART)
        r = pl.ds(pl.multiple_of((j % (rows // PART)) * PART, PART), PART)
        v = plain[s, r, :].astype(jnp.float32)
        w = v * cosine[r, :] + pltpu.roll(v, half, 1) * sine[r, :]
        turned[s, r, :] = w.astype(jnp.bfloat16)
        return 0

    lax.fori_loop(0, count * (rows // PART), turn, 0)

    def finish(ref, o):
        v = ref[o]
        out_keys[:, rows_of(o)] = v.T
        g = v.astype(jnp.float32).reshape(pages, PAGE, size)
        at = pl.ds(pl.multiple_of(o * pages, pages), pages)
        high[at, :] = jnp.max(g, axis=1)
        low[at, :] = jnp.min(g, axis=1)

    finish(turned, me)
    for kind in (1, 2):
        for dz in LATER:
            for dc in range(2):
                along(kind, ALONG.index((dz, dc))).start()
    for i in range(3):
        beside(1, i).start()
    for i in range(n):
        along(0, i).wait_recv()
        passed(0, i).start()

    @pl.when(between)
    def _():
        go_round().wait_recv()
        go_on().start()

    def overs(mine):
        @pl.when(mine)
        def _():
            for part in (0, 1):
                over(part).start()

        @pl.when(mine & jnp.logical_not(goes_round))
        def _():
            over(2).start()

    overs(z != 3)
    for j in range(RING - 2):
        for dc in range(2):
            last(j, dc).start()
    overs(z == 3)

    for i in range(n):
        along(1, i).wait_recv()
        passed(1, i).start()
    for i in range(3):
        beside(1, i).wait_recv()
        finish(landed, rank(*([mate] + across)[i]))
    for i in range(n):
        along(2, i).wait_recv()
        finish(landed, origin(i, x))
    for i in range(n):
        passed(1, i).wait_recv()
        finish(landed, origin(i, 1 - x))
    out_high[...] = high[...].astype(jnp.bfloat16)
    out_low[...] = low[...].astype(jnp.bfloat16)

    put_own.wait()
    for i in range(3):
        beside(0, i).wait_recv()
        for what in range(2):
            beside(what, i).wait_send()
    for i in range(n):
        passed(0, i).wait_recv()
        for kind in range(2):
            passed(kind, i).wait_send()
        for kind in range(3):
            along(kind, i).wait_send()
    @pl.when(goes_round)
    def _():
        go_round().wait_send()

    @pl.when(jnp.logical_not(goes_round))
    def _():
        over(2).wait_send()

    @pl.when(between)
    def _():
        go_on().wait_send()

    for part in (0, 1):
        over(part).wait_send()
    for part in (0, 1, 2):
        over_from(part).wait_recv()
    for i in range(n):
        if ALONG[i][0] != RING // 2:
            last_from(i).wait_recv()
    for j in range(RING - 2):
        for dc in range(2):
            last(j, dc).wait_send()


def store(*refs):
    n = len(PIECES)
    sources, targets, sem = refs[:n], refs[n : 2 * n], refs[2 * n]
    copies = []
    for src, dst, pieces in zip(sources, targets, PIECES):
        rows = src.shape[0] // pieces
        for p in range(pieces):
            at = pl.ds(p * rows, rows)
            copies.append(
                pltpu.make_async_copy(src.at[at], dst.at[at], sem.at[len(copies)])
            )
    for c in copies:
        c.start()
    for c in copies:
        c.wait()


def body(fresh_keys, fresh_values, turn_angle):
    count, rows, _, size = fresh_keys.shape
    length = count * rows
    n = len(ALONG)
    plain = (count, rows, size)
    vmem = pl.BlockSpec(memory_space=pltpu.VMEM)
    hbm = pl.BlockSpec(memory_space=pl.ANY)
    dma = pltpu.SemaphoreType.DMA
    out = pl.pallas_call(
        exchange,
        out_shape=[
            jax.ShapeDtypeStruct((size, length), jnp.bfloat16),
            jax.ShapeDtypeStruct((length, size), jnp.bfloat16),
            jax.ShapeDtypeStruct((length // PAGE, size), jnp.bfloat16),
            jax.ShapeDtypeStruct((length // PAGE, size), jnp.bfloat16),
        ],
        in_specs=[hbm] * 3,
        out_specs=[vmem] * 4,
        scratch_shapes=[
            pltpu.VMEM(plain, jnp.bfloat16),
            pltpu.VMEM(plain, jnp.bfloat16),
            pltpu.VMEM(plain, jnp.bfloat16),
            pltpu.VMEM((2, n, rows, size), jnp.bfloat16),
            pltpu.VMEM((size // 2, rows), jnp.float32),
            pltpu.VMEM((rows, size), jnp.float32),
            pltpu.VMEM((rows, size), jnp.float32),
            pltpu.VMEM((length // PAGE, size), jnp.float32),
            pltpu.VMEM((length // PAGE, size), jnp.float32),
            dma((3,)),
            dma((3 * n + 6,)),
            dma((3 * n + 6,)),
            dma((2 * n,)),
            dma((2 * n,)),
            dma((2 * (RING - 2),)),
            dma((2 * RING,)),
            pltpu.SemaphoreType.REGULAR((4,)),
            pltpu.SemaphoreType.REGULAR((RING // 2 - 1, 2)),
            pltpu.VMEM((2, 2, rows, size), jnp.bfloat16),
            dma((2, 2)),
            pltpu.VMEM((DETOUR, size), jnp.bfloat16),
            dma((5,)),
            dma((4,)),
        ],
        compiler_params=pltpu.CompilerParams(
            collective_id=0, has_side_effects=True, vmem_limit_bytes=44 << 20
        ),
        name="exchange",
    )(fresh_keys.reshape(plain), fresh_values.reshape(plain), turn_angle.T)
    keys, values, high, low = pl.pallas_call(
        store,
        out_shape=[jax.ShapeDtypeStruct(o.shape, o.dtype) for o in out],
        in_specs=[vmem] * 4,
        out_specs=[hbm] * 4,
        scratch_shapes=[dma((sum(PIECES),))],
        compiler_params=pltpu.CompilerParams(vmem_limit_bytes=1 << 20),
        name="store",
    )(*out)
    return (
        keys[None, None],
        values.reshape(1, length, 1, size),
        high.reshape(1, length // PAGE, 1, size),
        low.reshape(1, length // PAGE, 1, size),
    )


def solution(mesh):
    placed = (
        P(None, ("block", "span"), "model", None),
        P(None, ("block", "span"), "model", None),
        P(),
    )
    return jax.shard_map(
        body,
        mesh=mesh,
        in_specs=placed,
        out_specs=(
            P(("block", "span"), "model", None, None),
            P(("block", "span"), None, "model", None),
            P(("block", "span"), None, "model", None),
            P(("block", "span"), None, "model", None),
        ),
        check_vma=False,
    )
```

```python
import functools

import jax
import jax.numpy as jnp
from jax import lax
from jax.experimental import pallas as pl
from jax.experimental.pallas import tpu as pltpu
from jax.sharding import PartitionSpec as P

PAGE = 64
MESH = pl.DeviceIdType.MESH
RING = 8
PIECES = (4, 4, 1, 1)
EARLY = (1, 7, 2, 6, 3, 5, 4)
LATER = (3, 5, 1, 7, 4, 2, 6)
FINAL = (
    (7, 5, 6, 3, 2, 1),
    (0, 4, 7, 6, 2, 3),
    (0, 1, 7, 5, 4, 3),
    (0, 1, 2, 6, 5, 4),
    (1, 2, 7, 3, 6, 5),
    (0, 7, 2, 6, 3, 4),
    (0, 3, 1, 4, 5, 7),
    (0, 1, 4, 2, 5, 6),
)
ALONG = tuple((dz, dc) for dz in EARLY for dc in range(2))
DETOUR = 192
PART = 128


def place(core, x, z, model):
    return ((z % 2) * 4 + x * 2 + core, z // 2, model)


def rank(core, x, z):
    return ((z % 2) * 4 + x * 2 + core) * 4 + z // 2


def exchange(
    keys, values, angle, out_keys, out_values, out_high, out_low,
    plain, turned, landed, relay, angles, cosine, sine, high, low,
    load_sem, send_sem, recv_sem, pass_send_sem, pass_recv_sem, last_send_sem, last_recv_sem,
    inside, known, by_way, staged, stage_sem, detour, far_send_sem, far_recv_sem,
):
    block, span, model = (lax.axis_index(a) for a in ("block", "span", "model"))
    core, x, z = block % 2, (block // 2) % 2, span * 2 + block // 4
    me = rank(core, x, z)
    count, rows, size = plain.shape
    pages = rows // PAGE
    half = size // 2
    n = len(ALONG)

    def remote(src, dst, ssem, rsem, to):
        return pltpu.make_async_remote_copy(
            src, dst, ssem, rsem, device_id=place(*to, model), device_id_type=MESH
        )

    def signal(sem, *devices):
        for to in devices:
            pl.semaphore_signal(sem, inc=1, device_id=place(*to, model), device_id_type=MESH)

    def rows_of(r):
        return pl.ds(pl.multiple_of(r * rows, rows), rows)

    peers = [((core + dc) % 2, x, (z + dz) % RING) for dz, dc in ALONG]
    mate = (1 - core, x, z)
    across = [(c, 1 - x, z) for c in (core, 1 - core)]
    ahead = [(c, x, (z + 1) % RING) for c in (core, 1 - core)]
    behind = [(c, x, (z + RING - 1) % RING) for c in (core, 1 - core)]

    def sends_to(dz):
        return [i for i, (d, _) in enumerate(ALONG) if d == dz]

    first_of_ahead = z <= 5
    first_of_behind = (z == 0) | (z == 7)
    leaf = (z == 4) | (z == 7)
    hub = (z == 3) | (z == 0)
    first_of_across = (x == 0) & jnp.logical_not(leaf)
    second_of_across = (x == 1) & jnp.logical_not(leaf)
    first_of_mate = core == 1
    barrier = pltpu.get_barrier_semaphore()

    @pl.when(first_of_ahead)
    def _():
        signal(barrier, *ahead)

    @pl.when(first_of_behind)
    def _():
        signal(barrier, *behind)

    @pl.when(first_of_across)
    def _():
        signal(barrier, *across)

    @pl.when(first_of_mate)
    def _():
        signal(barrier, mate)

    def stage(side, i):
        c2, _, z2 = peers[i]
        return pltpu.make_async_copy(
            values.at[rank(c2, 1 - x, z2)], staged.at[side, ALONG[i][1]], stage_sem.at[side, ALONG[i][1]]
        )

    @pl.when(first_of_ahead)
    def _():
        for i in sends_to(1):
            stage(0, i).start()

    @pl.when(first_of_behind)
    def _():
        for i in sends_to(RING - 1):
            stage(1, i).start()

    get_angle = pltpu.make_async_copy(angle.at[:, rows_of(me)], angles, load_sem.at[0])
    get_angle.start()
    get_keys = pltpu.make_async_copy(keys, plain, load_sem.at[1])
    get_keys.start()
    put_own = pltpu.make_async_copy(values.at[me], out_values.at[rows_of(me)], load_sem.at[2])
    put_own.start()

    def along(kind, i, src=None):
        c2, _, z2 = to = peers[i]
        final = rank(c2, 1 - x if kind < 2 else x, z2)
        if src is None:
            src = (values if kind == 0 else turned).at[final]
        dst = relay.at[kind, i] if kind < 2 else landed.at[me]
        return remote(src, dst, send_sem.at[kind * n + i], recv_sem.at[kind * n + i], to)

    def beside(what, i):
        to = ([mate] + across)[i]
        at = 3 * n + what * 3 + i
        src = (values if what == 0 else turned).at[rank(*to)]
        dst = out_values.at[rows_of(me)] if what == 0 else landed.at[me]
        return remote(src, dst, send_sem.at[at], recv_sem.at[at], to)

    def origin(i, column):
        dz, dc = ALONG[i]
        return rank((core - dc) % 2, column, (z - dz) % RING)

    def passed(kind, i):
        dst = out_values.at[rows_of(origin(i, x))] if kind == 0 else landed.at[origin(i, x)]
        return remote(
            relay.at[kind, i], dst, pass_send_sem.at[kind * n + i], pass_recv_sem.at[kind * n + i],
            across[0],
        )


    def last(j, dc):
        to = ((core + dc) % 2, x, sum(jnp.where(z == k, t[j], 0) for k, t in enumerate(FINAL)))
        return remote(
            values.at[rank(*to)], out_values.at[rows_of(me)],
            last_send_sem.at[2 * j + dc], last_recv_sem.at[2 * z + core], to,
        )

    opposite = (z + RING // 2) % RING
    goes_round = (z == 1) | (z == 6)
    between = (z == 3) | (z == 4)
    front, back = pl.ds(0, rows - DETOUR), pl.ds(rows - DETOUR, DETOUR)

    def back_of(r):
        return pl.ds(pl.multiple_of(r * rows + rows - DETOUR, 64), DETOUR)

    def over(part):
        to = (1 - core if part == 0 else core, x, opposite)
        src = values.at[rank(*to)]
        if part == 0:
            dst = out_values.at[rows_of(me)]
        elif part == 1:
            src, dst = src.at[front], out_values.at[pl.ds(pl.multiple_of(me * rows, rows), rows - DETOUR)]
        else:
            src, dst = src.at[back], out_values.at[back_of(me)]
        return remote(src, dst, far_send_sem.at[part], far_recv_sem.at[part], to)

    def over_from(part):
        o = rank(1 - core if part == 0 else core, x, opposite)
        if part == 0:
            src = out_values.at[rows_of(o)]
        elif part == 1:
            src = out_values.at[pl.ds(pl.multiple_of(o * rows, rows), rows - DETOUR)]
        else:
            src = out_values.at[back_of(o)]
        return remote(src, src, far_send_sem.at[part], far_recv_sem.at[part], (core, x, opposite))

    def go_round():
        final = rank(core, x, opposite)
        return remote(
            values.at[final, back], detour, far_send_sem.at[3], far_recv_sem.at[3],
            (core, x, jnp.where(z == 6, 4, 3)),
        )

    def go_on():
        o = rank(core, x, jnp.where(z == 4, 6, 1))
        return remote(
            detour, out_values.at[back_of(o)], far_send_sem.at[4], far_recv_sem.at[2],
            (core, x, jnp.where(z == 4, 2, 5)),
        )

    def last_from(i):
        dz, dc = ALONG[i]
        at = 2 * ((z - dz) % RING) + (core - dc) % 2
        src = out_values.at[rows_of(origin(i, x))]
        return remote(src, src, last_send_sem.at[0], last_recv_sem.at[at], peers[i])

    due = jnp.where(z == 6, 4, jnp.where(z == 0, 0, 2)) + jnp.where(leaf, 0, 2 * x) + 1 - core

    @pl.when(due > 0)
    def _():
        pl.semaphore_wait(barrier, due)

    def first_sends(dz):
        for i in sends_to(dz):
            along(0, i).start()

    def staged_sends(side, dz):
        for i in sends_to(dz):
            stage(side, i).wait()
            along(0, i, staged.at[side, ALONG[i][1]]).start()

    @pl.when(jnp.logical_not(first_of_behind))
    def _():
        first_sends(RING - 1)
        signal(inside.at[0], *behind)

    @pl.when(jnp.logical_not(first_of_ahead))
    def _():
        first_sends(1)
        signal(inside.at[1], *ahead)

    @pl.when(second_of_across)
    def _():
        signal(inside.at[2], *across)

    @pl.when(jnp.logical_not(first_of_mate))
    def _():
        signal(inside.at[3], mate)

    @pl.when(first_of_ahead)
    def _():
        pl.semaphore_wait(inside.at[0], 2)
        staged_sends(0, 1)

    @pl.when(first_of_behind)
    def _():
        pl.semaphore_wait(inside.at[1], 2)
        staged_sends(1, RING - 1)

    far = RING // 2
    for step in range(1, far):
        signal(known.at[step - 1, 0], ahead[0])
        if step < far - 1:
            signal(known.at[step - 1, 1], behind[0])
        pl.semaphore_wait(known.at[step - 1, 0], 1)
        if step < far - 1:
            pl.semaphore_wait(known.at[step - 1, 1], 1)
        for dz in sorted({step + 1, RING - step - 1}):
            first_sends(dz)

    @pl.when(goes_round)
    def _():
        go_round().start()

    @pl.when(first_of_across)
    def _():
        pl.semaphore_wait(inside.at[2], 2)

    @pl.when(hub)
    def _():
        signal(by_way.at[0], across[0])
        pl.semaphore_wait(by_way.at[0], 1)
        signal(by_way.at[1], (core, x, jnp.where(z == 0, 7, 4)))

    @pl.when(leaf)
    def _():
        pl.semaphore_wait(by_way.at[1], 1)

    @pl.when(first_of_mate)
    def _():
        pl.semaphore_wait(inside.at[3], 1)

    for i in range(3):
        beside(0, i).start()

    get_angle.wait()
    a = angles[...]
    ca, sa = jnp.cos(a), jnp.sin(a)
    cosine[...] = jnp.concatenate([ca, ca], axis=0).T
    sine[...] = jnp.concatenate([-sa, sa], axis=0).T
    get_keys.wait()

    def turn(j, _):
        s = j // (rows // PART)
        r = pl.ds(pl.multiple_of((j % (rows // PART)) * PART, PART), PART)
        v = plain[s, r, :].astype(jnp.float32)
        w = v * cosine[r, :] + pltpu.roll(v, half, 1) * sine[r, :]
        turned[s, r, :] = w.astype(jnp.bfloat16)
        return 0

    lax.fori_loop(0, count * (rows // PART), turn, 0)

    def finish(ref, o):
        v = ref[o]
        out_keys[:, rows_of(o)] = v.T
        g = v.astype(jnp.float32).reshape(pages, PAGE, size)
        at = pl.ds(pl.multiple_of(o * pages, pages), pages)
        high[at, :] = jnp.max(g, axis=1)
        low[at, :] = jnp.min(g, axis=1)

    finish(turned, me)
    for kind in (1, 2):
        for dz in LATER:
            for dc in range(2):
                along(kind, ALONG.index((dz, dc))).start()
    for i in range(3):
        beside(1, i).start()
    for i in range(n):
        along(0, i).wait_recv()
        passed(0, i).start()

    @pl.when(between)
    def _():
        go_round().wait_recv()
        go_on().start()

    def overs(mine):
        @pl.when(mine)
        def _():
            for part in (0, 1):
                over(part).start()

        @pl.when(mine & jnp.logical_not(goes_round))
        def _():
            over(2).start()

    overs(z != 3)
    for j in range(RING - 2):
        for dc in range(2):
            last(j, dc).start()
    overs(z == 3)

    for i in range(n):
        along(1, i).wait_recv()
        passed(1, i).start()
    for i in range(3):
        beside(1, i).wait_recv()
        finish(landed, rank(*([mate] + across)[i]))
    for i in range(n):
        along(2, i).wait_recv()
        finish(landed, origin(i, x))
    for i in range(n):
        passed(1, i).wait_recv()
        finish(landed, origin(i, 1 - x))
    out_high[...] = high[...].astype(jnp.bfloat16)
    out_low[...] = low[...].astype(jnp.bfloat16)

    put_own.wait()
    for i in range(3):
        beside(0, i).wait_recv()
        for what in range(2):
            beside(what, i).wait_send()
    for i in range(n):
        passed(0, i).wait_recv()
        for kind in range(2):
            passed(kind, i).wait_send()
        for kind in range(3):
            along(kind, i).wait_send()
    @pl.when(goes_round)
    def _():
        go_round().wait_send()

    @pl.when(jnp.logical_not(goes_round))
    def _():
        over(2).wait_send()

    @pl.when(between)
    def _():
        go_on().wait_send()

    for part in (0, 1):
        over(part).wait_send()
    for part in (0, 1, 2):
        over_from(part).wait_recv()
    for i in range(n):
        if ALONG[i][0] != RING // 2:
            last_from(i).wait_recv()
    for j in range(RING - 2):
        for dc in range(2):
            last(j, dc).wait_send()


def store(*refs):
    n = len(PIECES)
    sources, targets, sem = refs[:n], refs[n : 2 * n], refs[2 * n]
    copies = []
    for src, dst, pieces in zip(sources, targets, PIECES):
        rows = src.shape[0] // pieces
        for p in range(pieces):
            at = pl.ds(p * rows, rows)
            copies.append(
                pltpu.make_async_copy(src.at[at], dst.at[at], sem.at[len(copies)])
            )
    for c in copies:
        c.start()
    for c in copies:
        c.wait()


def body(fresh_keys, fresh_values, turn_angle):
    count, rows, _, size = fresh_keys.shape
    length = count * rows
    n = len(ALONG)
    plain = (count, rows, size)
    vmem = pl.BlockSpec(memory_space=pltpu.VMEM)
    hbm = pl.BlockSpec(memory_space=pl.ANY)
    dma = pltpu.SemaphoreType.DMA
    out = pl.pallas_call(
        exchange,
        out_shape=[
            jax.ShapeDtypeStruct((size, length), jnp.bfloat16),
            jax.ShapeDtypeStruct((length, size), jnp.bfloat16),
            jax.ShapeDtypeStruct((length // PAGE, size), jnp.bfloat16),
            jax.ShapeDtypeStruct((length // PAGE, size), jnp.bfloat16),
        ],
        in_specs=[hbm] * 3,
        out_specs=[vmem] * 4,
        scratch_shapes=[
            pltpu.VMEM(plain, jnp.bfloat16),
            pltpu.VMEM(plain, jnp.bfloat16),
            pltpu.VMEM(plain, jnp.bfloat16),
            pltpu.VMEM((2, n, rows, size), jnp.bfloat16),
            pltpu.VMEM((size // 2, rows), jnp.float32),
            pltpu.VMEM((rows, size), jnp.float32),
            pltpu.VMEM((rows, size), jnp.float32),
            pltpu.VMEM((length // PAGE, size), jnp.float32),
            pltpu.VMEM((length // PAGE, size), jnp.float32),
            dma((3,)),
            dma((3 * n + 6,)),
            dma((3 * n + 6,)),
            dma((2 * n,)),
            dma((2 * n,)),
            dma((2 * (RING - 2),)),
            dma((2 * RING,)),
            pltpu.SemaphoreType.REGULAR((4,)),
            pltpu.SemaphoreType.REGULAR((RING // 2 - 1, 2)),
            pltpu.SemaphoreType.REGULAR((2,)),
            pltpu.VMEM((2, 2, rows, size), jnp.bfloat16),
            dma((2, 2)),
            pltpu.VMEM((DETOUR, size), jnp.bfloat16),
            dma((5,)),
            dma((4,)),
        ],
        compiler_params=pltpu.CompilerParams(
            collective_id=0, has_side_effects=True, vmem_limit_bytes=44 << 20
        ),
        name="exchange",
    )(fresh_keys.reshape(plain), fresh_values.reshape(plain), turn_angle.T)
    keys, values, high, low = pl.pallas_call(
        store,
        out_shape=[jax.ShapeDtypeStruct(o.shape, o.dtype) for o in out],
        in_specs=[vmem] * 4,
        out_specs=[hbm] * 4,
        scratch_shapes=[dma((sum(PIECES),))],
        compiler_params=pltpu.CompilerParams(vmem_limit_bytes=1 << 20),
        name="store",
    )(*out)
    return (
        keys[None, None],
        values.reshape(1, length, 1, size),
        high.reshape(1, length // PAGE, 1, size),
        low.reshape(1, length // PAGE, 1, size),
    )


def solution(mesh):
    placed = (
        P(None, ("block", "span"), "model", None),
        P(None, ("block", "span"), "model", None),
        P(),
    )
    return jax.shard_map(
        body,
        mesh=mesh,
        in_specs=placed,
        out_specs=(
            P(("block", "span"), "model", None, None),
            P(("block", "span"), None, "model", None),
            P(("block", "span"), None, "model", None),
            P(("block", "span"), None, "model", None),
        ),
        check_vma=False,
    )
```

```python
import functools

import jax
import jax.numpy as jnp
from jax import lax
from jax.experimental import pallas as pl
from jax.experimental.pallas import tpu as pltpu
from jax.sharding import PartitionSpec as P

PAGE = 64
MESH = pl.DeviceIdType.MESH
RING = 8
PIECES = (4, 4, 1, 1)
EARLY = (1, 7, 2, 6, 3, 5, 4)
LATER = (3, 5, 1, 7, 4, 2, 6)
FINAL = (
    (7, 5, 6, 3, 2, 1),
    (0, 4, 7, 6, 2, 3),
    (0, 1, 7, 5, 4, 3),
    (0, 1, 2, 6, 5, 4),
    (1, 2, 7, 3, 6, 5),
    (0, 7, 2, 6, 3, 4),
    (0, 3, 1, 4, 5, 7),
    (0, 1, 4, 2, 5, 6),
)
ALONG = tuple((dz, dc) for dz in EARLY for dc in range(2))
DETOUR = 192
PART = 128


def place(core, x, z, model):
    return ((z % 2) * 4 + x * 2 + core, z // 2, model)


def rank(core, x, z):
    return ((z % 2) * 4 + x * 2 + core) * 4 + z // 2


def exchange(
    keys, values, angle, out_keys, out_values, out_high, out_low,
    plain, turned, landed, relay, angles, cosine, sine, high, low,
    load_sem, send_sem, recv_sem, pass_send_sem, pass_recv_sem, last_send_sem, last_recv_sem,
    inside, known, by_way, staged, stage_sem, detour, far_send_sem, far_recv_sem,
):
    block, span, model = (lax.axis_index(a) for a in ("block", "span", "model"))
    core, x, z = block % 2, (block // 2) % 2, span * 2 + block // 4
    me = rank(core, x, z)
    count, rows, size = plain.shape
    pages = rows // PAGE
    half = size // 2
    n = len(ALONG)

    def remote(src, dst, ssem, rsem, to):
        return pltpu.make_async_remote_copy(
            src, dst, ssem, rsem, device_id=place(*to, model), device_id_type=MESH
        )

    def signal(sem, *devices):
        for to in devices:
            pl.semaphore_signal(sem, inc=1, device_id=place(*to, model), device_id_type=MESH)

    def rows_of(r):
        return pl.ds(pl.multiple_of(r * rows, rows), rows)

    peers = [((core + dc) % 2, x, (z + dz) % RING) for dz, dc in ALONG]
    mate = (1 - core, x, z)
    across = [(c, 1 - x, z) for c in (core, 1 - core)]
    ahead = [(c, x, (z + 1) % RING) for c in (core, 1 - core)]
    behind = [(c, x, (z + RING - 1) % RING) for c in (core, 1 - core)]

    def sends_to(dz):
        return [i for i, (d, _) in enumerate(ALONG) if d == dz]

    first_of_ahead = z <= 5
    first_of_behind = (z == 0) | (z == 7)
    leaf = (z == 4) | (z == 7)
    hub = (z == 3) | (z == 0)
    first_of_across = (x == 0) & jnp.logical_not(leaf)
    second_of_across = (x == 1) & jnp.logical_not(leaf)
    first_of_mate = core == 1
    barrier = pltpu.get_barrier_semaphore()

    @pl.when(first_of_ahead)
    def _():
        signal(barrier, *ahead)

    @pl.when(first_of_behind)
    def _():
        signal(barrier, *behind)

    @pl.when(first_of_across)
    def _():
        signal(barrier, *across)

    @pl.when(first_of_mate)
    def _():
        signal(barrier, mate)

    def stage(side, i):
        c2, _, z2 = peers[i]
        return pltpu.make_async_copy(
            values.at[rank(c2, 1 - x, z2)], staged.at[side, ALONG[i][1]], stage_sem.at[side, ALONG[i][1]]
        )

    def along(kind, i, src=None):
        c2, _, z2 = to = peers[i]
        final = rank(c2, 1 - x if kind < 2 else x, z2)
        if src is None:
            src = (values if kind == 0 else turned).at[final]
        dst = relay.at[kind, i] if kind < 2 else landed.at[me]
        return remote(src, dst, send_sem.at[kind * n + i], recv_sem.at[kind * n + i], to)

    def beside(what, i):
        to = ([mate] + across)[i]
        at = 3 * n + what * 3 + i
        src = (values if what == 0 else turned).at[rank(*to)]
        dst = out_values.at[rows_of(me)] if what == 0 else landed.at[me]
        return remote(src, dst, send_sem.at[at], recv_sem.at[at], to)

    def origin(i, column):
        dz, dc = ALONG[i]
        return rank((core - dc) % 2, column, (z - dz) % RING)

    def passed(kind, i):
        dst = out_values.at[rows_of(origin(i, x))] if kind == 0 else landed.at[origin(i, x)]
        return remote(
            relay.at[kind, i], dst, pass_send_sem.at[kind * n + i], pass_recv_sem.at[kind * n + i],
            across[0],
        )


    def last(j, dc):
        to = ((core + dc) % 2, x, sum(jnp.where(z == k, t[j], 0) for k, t in enumerate(FINAL)))
        return remote(
            values.at[rank(*to)], out_values.at[rows_of(me)],
            last_send_sem.at[2 * j + dc], last_recv_sem.at[2 * z + core], to,
        )

    opposite = (z + RING // 2) % RING
    goes_round = (z == 1) | (z == 6)
    between = (z == 3) | (z == 4)
    front, back = pl.ds(0, rows - DETOUR), pl.ds(rows - DETOUR, DETOUR)

    def back_of(r):
        return pl.ds(pl.multiple_of(r * rows + rows - DETOUR, 64), DETOUR)

    def over(part):
        to = (1 - core if part == 0 else core, x, opposite)
        src = values.at[rank(*to)]
        if part == 0:
            dst = out_values.at[rows_of(me)]
        elif part == 1:
            src, dst = src.at[front], out_values.at[pl.ds(pl.multiple_of(me * rows, rows), rows - DETOUR)]
        else:
            src, dst = src.at[back], out_values.at[back_of(me)]
        return remote(src, dst, far_send_sem.at[part], far_recv_sem.at[part], to)

    def over_from(part):
        o = rank(1 - core if part == 0 else core, x, opposite)
        if part == 0:
            src = out_values.at[rows_of(o)]
        elif part == 1:
            src = out_values.at[pl.ds(pl.multiple_of(o * rows, rows), rows - DETOUR)]
        else:
            src = out_values.at[back_of(o)]
        return remote(src, src, far_send_sem.at[part], far_recv_sem.at[part], (core, x, opposite))

    def go_round():
        final = rank(core, x, opposite)
        return remote(
            values.at[final, back], detour, far_send_sem.at[3], far_recv_sem.at[3],
            (core, x, jnp.where(z == 6, 4, 3)),
        )

    def go_on():
        o = rank(core, x, jnp.where(z == 4, 6, 1))
        return remote(
            detour, out_values.at[back_of(o)], far_send_sem.at[4], far_recv_sem.at[2],
            (core, x, jnp.where(z == 4, 2, 5)),
        )

    def last_from(i):
        dz, dc = ALONG[i]
        at = 2 * ((z - dz) % RING) + (core - dc) % 2
        src = out_values.at[rows_of(origin(i, x))]
        return remote(src, src, last_send_sem.at[0], last_recv_sem.at[at], peers[i])

    due = jnp.where(z == 6, 4, jnp.where(z == 0, 0, 2)) + jnp.where(leaf, 0, 2 * x) + 1 - core

    @pl.when(due > 0)
    def _():
        pl.semaphore_wait(barrier, due)

    def first_sends(dz):
        for i in sends_to(dz):
            along(0, i).start()

    def staged_sends(side, dz):
        for i in sends_to(dz):
            stage(side, i).wait()
            along(0, i, staged.at[side, ALONG[i][1]]).start()

    @pl.when(jnp.logical_not(first_of_behind))
    def _():
        first_sends(RING - 1)
        signal(inside.at[0], *behind)

    @pl.when(jnp.logical_not(first_of_ahead))
    def _():
        first_sends(1)
        signal(inside.at[1], *ahead)

    @pl.when(second_of_across)
    def _():
        signal(inside.at[2], *across)

    @pl.when(jnp.logical_not(first_of_mate))
    def _():
        signal(inside.at[3], mate)

    @pl.when(first_of_ahead)
    def _():
        for i in sends_to(1):
            stage(0, i).start()

    @pl.when(first_of_behind)
    def _():
        for i in sends_to(RING - 1):
            stage(1, i).start()

    get_angle = pltpu.make_async_copy(angle.at[:, rows_of(me)], angles, load_sem.at[0])
    get_angle.start()
    get_keys = pltpu.make_async_copy(keys, plain, load_sem.at[1])
    get_keys.start()
    put_own = pltpu.make_async_copy(values.at[me], out_values.at[rows_of(me)], load_sem.at[2])
    put_own.start()

    @pl.when(first_of_ahead)
    def _():
        pl.semaphore_wait(inside.at[0], 2)
        staged_sends(0, 1)

    @pl.when(first_of_behind)
    def _():
        pl.semaphore_wait(inside.at[1], 2)
        staged_sends(1, RING - 1)

    far = RING // 2
    for step in range(1, far):
        signal(known.at[step - 1, 0], ahead[0])
        if step < far - 1:
            signal(known.at[step - 1, 1], behind[0])
        pl.semaphore_wait(known.at[step - 1, 0], 1)
        if step < far - 1:
            pl.semaphore_wait(known.at[step - 1, 1], 1)
        for dz in sorted({step + 1, RING - step - 1}):
            first_sends(dz)

    @pl.when(goes_round)
    def _():
        go_round().start()

    @pl.when(first_of_across)
    def _():
        pl.semaphore_wait(inside.at[2], 2)

    @pl.when(hub)
    def _():
        signal(by_way.at[0], across[0])
        pl.semaphore_wait(by_way.at[0], 1)
        signal(by_way.at[1], (core, x, jnp.where(z == 0, 7, 4)))

    @pl.when(leaf)
    def _():
        pl.semaphore_wait(by_way.at[1], 1)

    @pl.when(first_of_mate)
    def _():
        pl.semaphore_wait(inside.at[3], 1)

    for i in range(3):
        beside(0, i).start()

    get_angle.wait()
    a = angles[...]
    ca, sa = jnp.cos(a), jnp.sin(a)
    cosine[...] = jnp.concatenate([ca, ca], axis=0).T
    sine[...] = jnp.concatenate([-sa, sa], axis=0).T
    get_keys.wait()

    def turn(j, _):
        s = j // (rows // PART)
        r = pl.ds(pl.multiple_of((j % (rows // PART)) * PART, PART), PART)
        v = plain[s, r, :].astype(jnp.float32)
        w = v * cosine[r, :] + pltpu.roll(v, half, 1) * sine[r, :]
        turned[s, r, :] = w.astype(jnp.bfloat16)
        return 0

    lax.fori_loop(0, count * (rows // PART), turn, 0)

    def finish(ref, o):
        v = ref[o]
        out_keys[:, rows_of(o)] = v.T
        g = v.astype(jnp.float32).reshape(pages, PAGE, size)
        at = pl.ds(pl.multiple_of(o * pages, pages), pages)
        high[at, :] = jnp.max(g, axis=1)
        low[at, :] = jnp.min(g, axis=1)

    finish(turned, me)
    for kind in (1, 2):
        for dz in LATER:
            for dc in range(2):
                along(kind, ALONG.index((dz, dc))).start()
    for i in range(3):
        beside(1, i).start()
    for i in range(n):
        along(0, i).wait_recv()
        passed(0, i).start()

    @pl.when(between)
    def _():
        go_round().wait_recv()
        go_on().start()

    def overs(mine):
        @pl.when(mine)
        def _():
            for part in (0, 1):
                over(part).start()

        @pl.when(mine & jnp.logical_not(goes_round))
        def _():
            over(2).start()

    overs(z != 3)
    for j in range(RING - 2):
        for dc in range(2):
            last(j, dc).start()
    overs(z == 3)

    for i in range(n):
        along(1, i).wait_recv()
        passed(1, i).start()
    for i in range(3):
        beside(1, i).wait_recv()
        finish(landed, rank(*([mate] + across)[i]))
    for i in range(n):
        along(2, i).wait_recv()
        finish(landed, origin(i, x))
    for i in range(n):
        passed(1, i).wait_recv()
        finish(landed, origin(i, 1 - x))
    out_high[...] = high[...].astype(jnp.bfloat16)
    out_low[...] = low[...].astype(jnp.bfloat16)

    put_own.wait()
    for i in range(3):
        beside(0, i).wait_recv()
        for what in range(2):
            beside(what, i).wait_send()
    for i in range(n):
        passed(0, i).wait_recv()
        for kind in range(2):
            passed(kind, i).wait_send()
        for kind in range(3):
            along(kind, i).wait_send()
    @pl.when(goes_round)
    def _():
        go_round().wait_send()

    @pl.when(jnp.logical_not(goes_round))
    def _():
        over(2).wait_send()

    @pl.when(between)
    def _():
        go_on().wait_send()

    for part in (0, 1):
        over(part).wait_send()
    for part in (0, 1, 2):
        over_from(part).wait_recv()
    for i in range(n):
        if ALONG[i][0] != RING // 2:
            last_from(i).wait_recv()
    for j in range(RING - 2):
        for dc in range(2):
            last(j, dc).wait_send()


def store(*refs):
    n = len(PIECES)
    sources, targets, sem = refs[:n], refs[n : 2 * n], refs[2 * n]
    copies = []
    for src, dst, pieces in zip(sources, targets, PIECES):
        rows = src.shape[0] // pieces
        for p in range(pieces):
            at = pl.ds(p * rows, rows)
            copies.append(
                pltpu.make_async_copy(src.at[at], dst.at[at], sem.at[len(copies)])
            )
    for c in copies:
        c.start()
    for c in copies:
        c.wait()


def body(fresh_keys, fresh_values, turn_angle):
    count, rows, _, size = fresh_keys.shape
    length = count * rows
    n = len(ALONG)
    plain = (count, rows, size)
    vmem = pl.BlockSpec(memory_space=pltpu.VMEM)
    hbm = pl.BlockSpec(memory_space=pl.ANY)
    dma = pltpu.SemaphoreType.DMA
    out = pl.pallas_call(
        exchange,
        out_shape=[
            jax.ShapeDtypeStruct((size, length), jnp.bfloat16),
            jax.ShapeDtypeStruct((length, size), jnp.bfloat16),
            jax.ShapeDtypeStruct((length // PAGE, size), jnp.bfloat16),
            jax.ShapeDtypeStruct((length // PAGE, size), jnp.bfloat16),
        ],
        in_specs=[hbm] * 3,
        out_specs=[vmem] * 4,
        scratch_shapes=[
            pltpu.VMEM(plain, jnp.bfloat16),
            pltpu.VMEM(plain, jnp.bfloat16),
            pltpu.VMEM(plain, jnp.bfloat16),
            pltpu.VMEM((2, n, rows, size), jnp.bfloat16),
            pltpu.VMEM((size // 2, rows), jnp.float32),
            pltpu.VMEM((rows, size), jnp.float32),
            pltpu.VMEM((rows, size), jnp.float32),
            pltpu.VMEM((length // PAGE, size), jnp.float32),
            pltpu.VMEM((length // PAGE, size), jnp.float32),
            dma((3,)),
            dma((3 * n + 6,)),
            dma((3 * n + 6,)),
            dma((2 * n,)),
            dma((2 * n,)),
            dma((2 * (RING - 2),)),
            dma((2 * RING,)),
            pltpu.SemaphoreType.REGULAR((4,)),
            pltpu.SemaphoreType.REGULAR((RING // 2 - 1, 2)),
            pltpu.SemaphoreType.REGULAR((2,)),
            pltpu.VMEM((2, 2, rows, size), jnp.bfloat16),
            dma((2, 2)),
            pltpu.VMEM((DETOUR, size), jnp.bfloat16),
            dma((5,)),
            dma((4,)),
        ],
        compiler_params=pltpu.CompilerParams(
            collective_id=0, has_side_effects=True, vmem_limit_bytes=44 << 20
        ),
        name="exchange",
    )(fresh_keys.reshape(plain), fresh_values.reshape(plain), turn_angle.T)
    keys, values, high, low = pl.pallas_call(
        store,
        out_shape=[jax.ShapeDtypeStruct(o.shape, o.dtype) for o in out],
        in_specs=[vmem] * 4,
        out_specs=[hbm] * 4,
        scratch_shapes=[dma((sum(PIECES),))],
        compiler_params=pltpu.CompilerParams(vmem_limit_bytes=1 << 20),
        name="store",
    )(*out)
    return (
        keys[None, None],
        values.reshape(1, length, 1, size),
        high.reshape(1, length // PAGE, 1, size),
        low.reshape(1, length // PAGE, 1, size),
    )


def solution(mesh):
    placed = (
        P(None, ("block", "span"), "model", None),
        P(None, ("block", "span"), "model", None),
        P(),
    )
    return jax.shard_map(
        body,
        mesh=mesh,
        in_specs=placed,
        out_specs=(
            P(("block", "span"), "model", None, None),
            P(("block", "span"), None, "model", None),
            P(("block", "span"), None, "model", None),
            P(("block", "span"), None, "model", None),
        ),
        check_vma=False,
    )
```
